128 devices in a mesh: blk: 64 (over y_lo, z, x, core), rep: 2 (over y_hi).
Axes of the slice: x: 4, y: 4 (y_hi: 2, y_lo: 2; y = y_hi * 2 + y_lo), z: 4, core: 2. Of those that a mesh axis runs over, the one named last changes fastest.
Arguments:
- measured: float32 [3, 64, 8, 1536], P(None, 'blk', None, 'rep'), may hold values from -4 to 4
- rot_vector: float32 [3, 64, 8, 1536], P(None, 'blk', None, 'rep'), may hold values from -6 to 6
- confidence: float32 [3, 64, 8, 1536], P(None, 'blk', None, 'rep'), may hold values from 0.5 to 2
- first_local: int32 [64, 8, 1536], P('blk', None, 'rep'), may hold values from 0 to 2047
- second_local: int32 [64, 8, 1536], P('blk', None, 'rep'), may hold values from 0 to 2047
- edge_counts: int32 [64, 8, 2], P('blk', None, 'rep'), may hold values from 256 to 768, as said below
- start_angles: float32 [3, 131072], P(None, 'blk'), may hold values from -4 to 4
- anchor: float32 [131072], P('blk'), may hold values from 0.05 to 0.5
Outputs:
- estimate: float32 [3, 131072], P(None, 'blk')
- weights: float32 [64, 8, 1536], P('blk', None, 'rep')
The draws below stay inside these ranges and needn't reach their ends.
Inputs may be any that keep to these rules, and one draw needn't show every extreme that they name: `edge_counts`: live edges of a tile pair on one device fill its first slots; in every tile some pair holds 768 live edges on one device.
All inputs are finite; a program needn't handle non-finite values.
Results may differ from the reference program's by a relative error of at most 0.0001.
Values sent between devices are 32-bit elements; how exact they have to be, the bound alone decides.
A program may use at most 128 MiB of HBM per device.

```python
import math
import jax
import jax.numpy as jnp
from jax import lax

CT = 2048
EH = 768
OFFS = 8
PASSES = 2
ITERS = 2
NCAM = 131072
EPT = 1536
N_BLK = 64


def draw_edge_counts(key, part):
    tile_total = NCAM // CT
    halves = EPT // EH
    base_key, pair_key, half_key = jax.random.split(jax.random.fold_in(key, 11), 3)
    base = jax.random.randint(base_key, (tile_total, OFFS, halves), EH // 3, EH + 1, dtype=jnp.int32)
    pick_pair = jax.random.randint(pair_key, (tile_total, 1, 1), 0, OFFS, dtype=jnp.int32)
    pick_half = jax.random.randint(half_key, (tile_total, 1, 1), 0, halves, dtype=jnp.int32)
    chosen = (jnp.arange(OFFS, dtype=jnp.int32)[None, :, None] == pick_pair) & (jnp.arange(halves, dtype=jnp.int32)[None, None, :] == pick_half)
    return jnp.where(chosen, EH, base).astype(jnp.int32)


def draw_measured(key, part):
    tile_total = NCAM // CT
    shape = (3, tile_total, OFFS, EPT)
    rising = 1.0 + 2.0 * jnp.arange(tile_total, dtype=jnp.float32) / max(tile_total - 1, 1)
    rising = rising[None, :, None, None]
    value_key = jax.random.fold_in(jax.random.fold_in(key, 23), 0)
    return jnp.clip(0.3 * rising * jax.random.normal(value_key, shape, jnp.float32), -4.0, 4.0)


def with_ends(values, key, smallest, largest):
    longest = values.shape.index(max(values.shape))
    spots = []
    for shift in (0, 1):
        where = [jax.random.randint(jax.random.fold_in(key, axis), (), 0, length) for axis, length in enumerate(values.shape)]
        where[longest] = (where[longest] + shift) % values.shape[longest]
        spots.append(tuple(where))
    return values.at[spots[0]].set(smallest).at[spots[1]].set(largest)


def block_scale(own_key, dims, cuts, low, largest):
    level = 1.0
    for axis_at, blocks in cuts:
        draws = jax.random.uniform(jax.random.fold_in(jax.random.fold_in(own_key, 6), axis_at), (blocks,), jnp.float32, low / len(cuts), largest / len(cuts))
        level = level * jnp.repeat(jnp.exp(draws), dims[axis_at] // blocks).reshape((-1,) + (1,) * (len(dims) - 1 - axis_at))
    return level


def gaussian(key, shape, scale, limit, cuts=(), held_as=jnp.bfloat16):
    array = jax.random.normal(key, shape, jnp.float32) * scale
    if len(cuts) > 0:
        array = block_scale(key, shape, cuts, -0.22, 0.18) * array
    return jnp.clip(array, min=-limit, max=limit).astype(held_as)


def setup_inputs(seed: int = 0) -> dict:
    key_of = jax.random.split(jax.random.key(seed), 9)
    return {
        "measured": draw_measured(jax.random.fold_in(key_of[8], 71), 0),
        "rot_vector": gaussian(key_of[1], (3, N_BLK, OFFS, EPT), 1.0, 6.0, ((1, 64), (3, 2)), jnp.float32),
        "confidence": jnp.clip(jnp.exp(math.log(2.0) - 1.3862944 * jax.random.uniform(key_of[2], (3, N_BLK, OFFS, EPT), jnp.float32) ** block_scale(key_of[2], (3, N_BLK, OFFS, EPT), ((1, 64), (3, 2)), -0.2, 0.2)), 0.5, 2.0),
        "first_local": with_ends(jax.random.randint(key_of[3], (N_BLK, OFFS, EPT), 0, CT), jax.random.fold_in(key_of[3], 1), 0, CT - 1).astype(jnp.int32),
        "second_local": with_ends(jax.random.randint(key_of[4], (N_BLK, OFFS, EPT), 0, CT), jax.random.fold_in(key_of[4], 1), 0, CT - 1).astype(jnp.int32),
        "edge_counts": draw_edge_counts(jax.random.fold_in(key_of[8], 71), 0),
        "start_angles": gaussian(key_of[6], (3, NCAM), 0.3, 4.0, ((1, 64),), jnp.float32),
        "anchor": jnp.clip(jnp.exp(math.log(0.5) - 2.3025851 * jax.random.uniform(key_of[7], (NCAM,), jnp.float32) ** block_scale(key_of[7], (NCAM,), ((0, 64),), -0.2, 0.2)), 0.05, 0.5),
    }


PAIRS = ((0, 0), (0, 1), (0, 2), (1, 1), (1, 2), (2, 2))
LOOKUP = ((0, 1, 2), (1, 3, 4), (2, 4, 5))
SOFTEN = 0.05

def rotations(vector):
    squared = vector[0] * vector[0] + vector[1] * vector[1] + vector[2] * vector[2]
    factor = 2.0 / (1.0 + squared)
    zeros = jnp.zeros_like(squared)
    skewed = ((zeros, -vector[2], vector[1]), (vector[2], zeros, -vector[0]), (-vector[1], vector[0], zeros))
    matrix_rows = []
    for first in range(3):
        entries = []
        for second in range(3):
            term = skewed[first][second] + vector[first] * vector[second]
            if first == second:
                entries.append(1.0 + factor * (term - squared))
            else:
                entries.append(factor * term)
        matrix_rows.append(jnp.stack(entries))
    return jnp.stack(matrix_rows)

def rotate(rotation, vector):
    return lax.optimization_barrier(jnp.sum(rotation * vector[None], axis=1))

def rotate_back(rotation, vector):
    return lax.optimization_barrier(jnp.sum(rotation * vector[:, None], axis=0))

def block_parts(weighted, rotation):
    far_list = []
    near_list = []
    for first, second in PAIRS:
        near_list.append(lax.optimization_barrier(jnp.sum(rotation[:, first] * weighted * rotation[:, second], axis=0)))
        if first == second:
            far_list.append(weighted[first])
        else:
            far_list.append(jnp.zeros_like(weighted[0]))
    return (jnp.stack(far_list), jnp.stack(near_list))

def inverse_apply(blocks, vector):
    adjugate = jnp.stack([blocks[3] * blocks[5] - blocks[4] * blocks[4], blocks[2] * blocks[4] - blocks[1] * blocks[5], blocks[1] * blocks[4] - blocks[2] * blocks[3], blocks[0] * blocks[5] - blocks[2] * blocks[2], blocks[1] * blocks[2] - blocks[0] * blocks[4], blocks[0] * blocks[3] - blocks[1] * blocks[1]])
    determinant = blocks[0] * adjugate[0] + blocks[1] * adjugate[1] + blocks[2] * adjugate[2]
    result = []
    for first in range(3):
        total = adjugate[LOOKUP[first][0]] * vector[0] + adjugate[LOOKUP[first][1]] * vector[1] + adjugate[LOOKUP[first][2]] * vector[2]
        result.append(total / determinant)
    return jnp.stack(result)

def spread(terms, index, total):
    return jax.vmap(lambda values: jax.ops.segment_sum(values, index, num_segments=total))(terms)

def reference(measured, rot_vector, confidence, first_local, second_local, edge_counts, start_angles, anchor):
    tile_ids = jnp.arange(N_BLK, dtype=jnp.int32)[:, None, None]
    pair_ids = jnp.arange(OFFS, dtype=jnp.int32)[None, :, None]
    first = (tile_ids * CT + first_local).reshape(-1).astype(jnp.int32)
    second = ((tile_ids + pair_ids) % N_BLK * CT + second_local).reshape(-1).astype(jnp.int32)
    slots = jnp.arange(EPT, dtype=jnp.int32) % EH
    live = (slots[None, None, :] < jnp.repeat(edge_counts, EH, axis=2)).astype(jnp.float32).reshape(-1)
    measured = measured.reshape(3, -1)
    confidence = confidence.reshape(3, -1)
    rotation = rotations(rot_vector.reshape(3, -1))
    cameras = N_BLK * CT
    diagonal = jnp.stack([anchor if first_c == second_c else jnp.zeros_like(anchor) for first_c, second_c in PAIRS])

    def gather_back(terms):
        return spread(terms, second, cameras) - spread(rotate_back(rotation, terms), first, cameras)
    estimate = start_angles
    weights = live
    for sweep_index in range(PASSES):
        misfit = measured - (estimate[:, second] - rotate(rotation, estimate[:, first]))
        weights = live / jnp.sqrt(lax.optimization_barrier(jnp.sum(confidence * misfit * misfit, axis=0)) + SOFTEN * SOFTEN)
        weighted = weights * confidence
        residual = gather_back(weighted * misfit) - anchor * estimate
        far_part, near_part = block_parts(weighted, rotation)
        blocks = spread(far_part, second, cameras) + spread(near_part, first, cameras) + diagonal
        scaled = inverse_apply(blocks, residual)
        direction = scaled
        norm_now = jnp.sum(residual * scaled)
        for inner_index in range(ITERS):
            changed = direction[:, second] - rotate(rotation, direction[:, first])
            image = gather_back(weighted * changed) + anchor * direction
            step_size = norm_now / jnp.sum(direction * image)
            estimate = estimate + step_size * direction
            residual = residual - step_size * image
            if inner_index + 1 < ITERS:
                scaled = inverse_apply(blocks, residual)
                norm_next = jnp.sum(residual * scaled)
                direction = scaled + norm_next / norm_now * direction
                norm_now = norm_next
    return (estimate, weights.reshape(N_BLK, OFFS, EPT))
```

```python
import functools

import jax
import jax.numpy as jnp
from jax import lax
from jax.experimental import pallas as pl
from jax.experimental.pallas import tpu as pltpu
from jax.sharding import PartitionSpec as P

PASSES = 2
SOFTEN = 0.05
MESH = pl.DeviceIdType.MESH
LANES = 128
HI = 8
GROUP = 8
PAIRS = ((0, 0), (0, 1), (0, 2), (1, 1), (1, 2), (2, 2))
F32 = jnp.float32
BF16 = jnp.bfloat16


def dot_nn(a, b):
    return lax.dot_general(a, b, (((1,), (0,)), ((), ())), preferred_element_type=F32)


def dot_nt(a, b):
    return lax.dot_general(a, b, (((1,), (1,)), ((), ())), preferred_element_type=F32)


def two_pieces(value):
    high = value.astype(BF16).astype(F32)
    return high, value - high


def kernel(
    n_blk,
    n_rep,
    measured_ref,
    rot_ref,
    conf_ref,
    first_ref,
    second_ref,
    counts_ref,
    start_ref,
    anchor_ref,
    est_out,
    weights_out,
    hot,
    himask,
    idx,
    rotm,
    meas,
    conf,
    live,
    wout,
    mis,
    wconf,
    chz,
    chu,
    send1,
    recv1,
    send2,
    recv2,
    est,
    halo,
    anc,
    inv,
    fz,
    fu,
    fr,
    fq,
    bsend,
    brecv,
    dsend,
    drecv,
    xsend,
    xrecv,
    g1send,
    g1recv,
    g2send,
    g2recv,
    lhs,
    s_init,
    r_init,
    s_b,
    r_b,
    s_d,
    r_d,
    s_x,
    r_x,
    s_g1,
    r_g1,
    s_g2,
    r_g2,
):
    pairs = idx.shape[0] // 3
    tiles = idx.shape[1]
    lo_count = est.shape[2]
    outer = n_blk // GROUP
    wide = outer * n_rep
    b = lax.axis_index("blk")
    r = lax.axis_index("rep")
    low = lax.rem(b, GROUP)
    high = b // GROUP
    mine2 = high * n_rep + r

    def ahead(k):
        return lax.rem(b + k, n_blk)

    def behind(k):
        return lax.rem(b + n_blk - k, n_blk)

    def copy(src, dst, send, recv, blk, rep):
        return pltpu.make_async_remote_copy(
            src_ref=src,
            dst_ref=dst,
            send_sem=send,
            recv_sem=recv,
            device_id={"blk": blk, "rep": rep},
            device_id_type=MESH,
        )

    barrier = pltpu.get_barrier_semaphore()

    def greet(blk, rep):
        pl.semaphore_signal(barrier, inc=1, device_id={"blk": blk, "rep": rep}, device_id_type=MESH)

    def greet_pairs(k, _):
        greet(ahead(k), r)
        greet(behind(k), r)
        return 0

    lax.fori_loop(1, pairs, greet_pairs, 0)
    greet(b, 1 - r)

    def inner_peer(j):
        return high * GROUP + lax.rem(low + j, GROUP)

    def outer_peer(j):
        other = lax.rem(mine2 + j, wide)
        return (other // n_rep) * GROUP + low, lax.rem(other, n_rep)

    def greet_inner(j, _):
        greet(inner_peer(j), r)
        return 0

    def greet_outer(j, _):
        blk, rep = outer_peer(j)
        greet(blk, rep)
        return 0

    lax.fori_loop(1, GROUP, greet_inner, 0)
    lax.fori_loop(1, wide, greet_outer, 0)

    def lanes_of(t):
        return pl.ds(t * LANES, LANES)

    live_all = lax.broadcasted_iota(jnp.int32, first_ref.shape[1:], 1) < counts_ref[0]
    live_all = jnp.where(live_all, 1.0, 0.0).astype(F32)
    for k in range(pairs):
        for t in range(tiles):
            at = slice(t * LANES, (t + 1) * LANES)
            live[k, t : t + 1] = live_all[k : k + 1, at]
            idx[k, t : t + 1] = first_ref[0, k : k + 1, at]
            idx[2 * pairs + k, t : t + 1] = second_ref[0, k : k + 1, at]
            for c in range(3):
                conf[k, c, t : t + 1] = conf_ref[c, 0, k : k + 1, at] * live_all[k : k + 1, at]
                meas[k, c, t : t + 1] = measured_ref[c, 0, k : k + 1, at]
                rotm[k, c, t : t + 1] = rot_ref[c, 0, k : k + 1, at]
    for h in range(HI):
        at = slice(h * lo_count, (h + 1) * lo_count)
        anc[h : h + 1] = anchor_ref[0:1, at]
        for c in range(3):
            est[c, h : h + 1] = start_ref[c : c + 1, at]

    def stage1(k, _):
        for c in range(3):
            send1[k, c] = conf[k, c]
        send1[k, 3] = idx[2 * pairs + k].astype(F32)
        return 0

    lax.fori_loop(0, pairs, stage1, 0)
    halo[0] = est[...]

    pl.semaphore_wait(barrier, 2 * (pairs - 1) + 1 + (GROUP - 1) + (wide - 1))

    def send_init(k):
        return copy(send1.at[k], recv1.at[k], s_init.at[0, k], r_init.at[0, k], ahead(k), r)

    def send_mis(k):
        return copy(send2.at[k], recv2.at[k], s_init.at[1, k], r_init.at[1, k], ahead(k), r)

    def send_halo(k):
        return copy(halo.at[0], halo.at[k], s_init.at[2, k], r_init.at[2, k], behind(k), r)

    def start_init(k, _):
        send_init(k).start()
        send_halo(k).start()
        return 0

    lax.fori_loop(1, pairs, start_init, 0)
    recv1[0] = send1[0]

    def rotations(k, _):
        v = [rotm[k, c] for c in range(3)]
        squared = v[0] * v[0] + v[1] * v[1] + v[2] * v[2]
        factor = 2.0 / (1.0 + squared)
        zero = jnp.zeros_like(squared)
        skew = ((zero, -v[2], v[1]), (v[2], zero, -v[0]), (-v[1], v[0], zero))
        for i in range(3):
            for j in range(3):
                term = skew[i][j] + v[i] * v[j]
                if i == j:
                    rotm[k, 3 * i + j] = 1.0 + factor * (term - squared)
                else:
                    rotm[k, 3 * i + j] = factor * term
        return 0

    lax.fori_loop(0, pairs, rotations, 0)

    def build(g):
        for t in range(tiles):
            where = idx[g, t : t + 1]
            low_part = lax.rem(where, lo_count)
            high_part = where // lo_count
            at = slice(t * LANES, (t + 1) * LANES)
            himask[g, :, at] = jnp.where(
                lax.broadcasted_iota(jnp.int32, (HI, LANES), 0) == high_part, 1.0, 0.0
            ).astype(F32)
            hot[g, :, at] = jnp.where(
                lax.broadcasted_iota(jnp.int32, (lo_count, LANES), 0) == low_part, 1.0, 0.0
            ).astype(BF16)

    def build_near(k, _):
        build(k)
        return 0

    def build_second(k, _):
        build(2 * pairs + k)
        return 0

    def table_of(field):
        rows = []
        for c in range(3):
            rows.extend(two_pieces(field[c]))
        return jnp.concatenate(rows, axis=0).astype(BF16)

    def gather(table, g):
        full = dot_nn(table, hot[g])
        mask = himask[g]
        found = []
        for c in range(3):
            part = (full[16 * c : 16 * c + 8] + full[16 * c + 8 : 16 * c + 16]) * mask
            row = jnp.sum(part, axis=0, keepdims=True)
            found.append(
                jnp.concatenate([row[:, t * LANES : (t + 1) * LANES] for t in range(tiles)], axis=0)
            )
        return found

    def rotate(k, vec):
        return [
            rotm[k, 3 * i] * vec[0] + rotm[k, 3 * i + 1] * vec[1] + rotm[k, 3 * i + 2] * vec[2]
            for i in range(3)
        ]

    def rotate_back(k, vec):
        return [
            rotm[k, i] * vec[0] + rotm[k, 3 + i] * vec[1] + rotm[k, 6 + i] * vec[2]
            for i in range(3)
        ]

    lax.fori_loop(0, pairs, build_near, 0)
    table = table_of(est)

    def near_start(i, _):
        k = lax.rem(i + 1, pairs)
        turned = rotate(k, gather(table, k))
        for c in range(3):
            send2[k, c] = meas[k, c] + turned[c]

        @pl.when(k != 0)
        def _():
            send_mis(k).start()

        return 0

    lax.fori_loop(0, pairs, near_start, 0)
    recv2[0] = send2[0]

    lax.fori_loop(0, pairs, build_second, 0)

    def wait_halo(k, _):
        copy(halo.at[0], halo.at[k], s_init.at[2, k], r_init.at[2, k], b, r).wait_recv()
        return 0

    lax.fori_loop(1, pairs, wait_halo, 0)

    def own_misfit(k, _):
        there = gather(table_of(halo.at[k]), 2 * pairs + k)
        for c in range(3):
            mis[0, k, c] = send2[k, c] - there[c]
        return 0

    lax.fori_loop(0, pairs, own_misfit, 0)

    def wait_init(k, _):
        copy(send1.at[k], recv1.at[k], s_init.at[0, k], r_init.at[0, k], b, r).wait_recv()
        return 0

    lax.fori_loop(1, pairs, wait_init, 0)

    def build_far(k, _):
        idx[pairs + k] = recv1[k, 3].astype(jnp.int32)
        build(pairs + k)
        return 0

    lax.fori_loop(0, pairs, build_far, 0)

    def wait_mis(k, _):
        copy(send2.at[k], recv2.at[k], s_init.at[1, k], r_init.at[1, k], b, r).wait_recv()
        return 0

    lax.fori_loop(1, pairs, wait_mis, 0)

    def far_misfit(k, _):
        there = gather(table, pairs + k)
        for c in range(3):
            mis[1, k, c] = recv2[k, c] - there[c]
        return 0

    lax.fori_loop(0, pairs, far_misfit, 0)

    def put(slot, at_row, terms, g):
        for n, term in enumerate(terms):
            head, tail = two_pieces(term)
            for t in range(tiles):
                at = slice(t * LANES, (t + 1) * LANES)
                mask = himask[g, :, at]
                both = jnp.concatenate([head[t : t + 1] * mask, tail[t : t + 1] * mask], axis=0)
                lhs[slot, at_row + 16 * n : at_row + 16 * n + 16, at] = both.astype(BF16)

    def summed(totals, channel):
        return totals[16 * channel : 16 * channel + 8] + totals[16 * channel + 8 : 16 * channel + 16]

    def full_sum(value):
        return jnp.sum(jnp.sum(value, axis=0, keepdims=True), axis=1, keepdims=True)

    def invert(vec_ref, out_ref):
        for i in range(3):
            look = ((0, 1, 2), (1, 3, 4), (2, 4, 5))[i]
            out_ref[i] = (
                inv[look[0]] * vec_ref[0] + inv[look[1]] * vec_ref[1] + inv[look[2]] * vec_ref[2]
            )

    def exchange_start(x, table):
        def step(i, _):
            k = lax.rem(i + 1, pairs)
            turned = rotate(k, gather(table, k))
            there = gather(table, pairs + k)
            for c in range(3):
                xsend[x, 0, k, c] = turned[c]
                xsend[x, 1, k, c] = there[c]

            @pl.when(k != 0)
            def _():
                send_back(x, k).start()
                send_ahead(x, k).start()

            return 0

        lax.fori_loop(0, pairs, step, 0)
        xrecv[x, 0, 0] = xsend[x, 0, 0]
        xrecv[x, 1, 0] = xsend[x, 1, 0]

    def send_ahead(x, k):
        return copy(xsend.at[x, 0, k], xrecv.at[x, 0, k], s_x.at[x, 0, k], r_x.at[x, 0, k], ahead(k), r)

    def send_back(x, k):
        return copy(xsend.at[x, 1, k], xrecv.at[x, 1, k], s_x.at[x, 1, k], r_x.at[x, 1, k], behind(k), r)

    def wait_exchange(x, k):
        @pl.when(k != 0)
        def _():
            copy(xsend.at[x, 1, k], xrecv.at[x, 1, k], s_x.at[x, 1, k], r_x.at[x, 1, k], b, r).wait_recv()
            copy(xsend.at[x, 0, k], xrecv.at[x, 0, k], s_x.at[x, 0, k], r_x.at[x, 0, k], b, r).wait_recv()

    lane = lax.broadcasted_iota(jnp.int32, (1, LANES), 1)

    for p in range(PASSES):
        def near_sums(k, totals):
            m = [mis[0, k, c] for c in range(3)]
            cf = [conf[k, c] for c in range(3)]
            squares = cf[0] * m[0] * m[0] + cf[1] * m[1] * m[1] + cf[2] * m[2] * m[2]
            weight = live[k] / jnp.sqrt(squares + SOFTEN * SOFTEN)
            wout[k] = weight
            wc = [weight * cf[c] for c in range(3)]
            for c in range(3):
                wconf[0, k, c] = wc[c]
            back = rotate_back(k, [wc[c] * m[c] for c in range(3)])
            rot = [[rotm[k, 3 * i + j] for j in range(3)] for i in range(3)]
            terms = [-value for value in back]
            for f, s in PAIRS:
                terms.append(
                    rot[0][f] * wc[0] * rot[0][s]
                    + rot[1][f] * wc[1] * rot[1][s]
                    + rot[2][f] * wc[2] * rot[2][s]
                )
            put(0, 0, terms, k)
            return totals + dot_nt(lhs[0], hot[k])

        def far_sums(k, totals):
            m = [mis[1, k, c] for c in range(3)]
            cf = [recv1[k, c] for c in range(3)]
            squares = cf[0] * m[0] * m[0] + cf[1] * m[1] * m[1] + cf[2] * m[2] * m[2]
            weight = 1.0 / jnp.sqrt(squares + SOFTEN * SOFTEN)
            wc = [weight * cf[c] for c in range(3)]
            for c in range(3):
                wconf[1, k, c] = wc[c]
            put(1, 0, [wc[c] * m[c] for c in range(3)] + wc, pairs + k)
            return totals + dot_nt(lhs[1, 0:96], hot[pairs + k])

        near = lax.fori_loop(0, pairs, near_sums, jnp.zeros((144, lo_count), F32))
        far = lax.fori_loop(0, pairs, far_sums, jnp.zeros((96, lo_count), F32))
        for n in range(9):
            total = summed(near, n)
            spot = {0: 0, 1: 1, 2: 2, 3: 3, 6: 4, 8: 5}.get(n)
            if spot is not None:
                total = total + summed(far, spot)
            bsend[p, n] = total
        copy(bsend.at[p], brecv.at[p], s_b.at[p], r_b.at[p], b, 1 - r).start()
        copy(bsend.at[p], brecv.at[p], s_b.at[p], r_b.at[p], b, 1 - r).wait_recv()
        anchor = anc[...]
        for c in range(3):
            fr[c] = bsend[p, c] + brecv[p, c] - anchor * est[c]
        blocks = []
        for n, (f, s) in enumerate(PAIRS):
            block = bsend[p, 3 + n] + brecv[p, 3 + n]
            blocks.append(block + anchor if f == s else block)
        adjugate = [
            blocks[3] * blocks[5] - blocks[4] * blocks[4],
            blocks[2] * blocks[4] - blocks[1] * blocks[5],
            blocks[1] * blocks[4] - blocks[2] * blocks[3],
            blocks[0] * blocks[5] - blocks[2] * blocks[2],
            blocks[1] * blocks[2] - blocks[0] * blocks[4],
            blocks[0] * blocks[3] - blocks[1] * blocks[1],
        ]
        determinant = blocks[0] * adjugate[0] + blocks[1] * adjugate[1] + blocks[2] * adjugate[2]
        for n in range(6):
            inv[n] = adjugate[n] / determinant
        invert(fr, fz)

        x = 2 * p
        exchange_start(x, table_of(fz))

        def product_near(k, totals):
            wait_exchange(x, k)
            change = [xrecv[x, 1, k, c] - xsend[x, 0, k, c] for c in range(3)]
            pushed = []
            square = totals[1]
            for c in range(3):
                chz[0, k, c] = change[c]
                pushed.append(wconf[0, k, c] * change[c])
                square = square + pushed[c] * change[c]
            put(0, 0, [-value for value in rotate_back(k, pushed)], k)
            return totals[0] + dot_nt(lhs[0, 0:48], hot[k]), square

        def product_far(k, totals):
            change = [xsend[x, 1, k, c] - xrecv[x, 0, k, c] for c in range(3)]
            pushed = []
            for c in range(3):
                chz[1, k, c] = change[c]
                pushed.append(wconf[1, k, c] * change[c])
            put(1, 0, pushed, pairs + k)
            return totals + dot_nt(lhs[1, 0:48], hot[pairs + k])

        zero_row = jnp.zeros((tiles, LANES), F32)
        totals, z_square = lax.fori_loop(
            0, pairs, product_near, (jnp.zeros((48, lo_count), F32), zero_row)
        )
        totals = lax.fori_loop(0, pairs, product_far, totals)
        for c in range(3):
            dsend[p, c] = summed(totals, c)
        copy(dsend.at[p], drecv.at[p], s_d.at[p], r_d.at[p], b, 1 - r).start()
        copy(dsend.at[p], drecv.at[p], s_d.at[p], r_d.at[p], b, 1 - r).wait_recv()
        for c in range(3):
            fq[c] = dsend[p, c] + drecv[p, c] + anchor * fz[c]
        invert(fq, fu)

        y = 2 * p + 1
        exchange_start(y, table_of(fu))

        def change_u(k, square):
            wait_exchange(y, k)
            for c in range(3):
                change = xrecv[y, 1, k, c] - xsend[y, 0, k, c]
                chu[0, k, c] = change
                square = square + wconf[0, k, c] * change * change
                chu[1, k, c] = xsend[y, 1, k, c] - xrecv[y, 0, k, c]
            return square

        u_square = lax.fori_loop(0, pairs, change_u, zero_row)

        half = 1.0 / n_rep
        rz = fr[0] * fz[0] + fr[1] * fz[1] + fr[2] * fz[2]
        zz = anchor * (fz[0] * fz[0] + fz[1] * fz[1] + fz[2] * fz[2])
        uu = anchor * (fu[0] * fu[0] + fu[1] * fu[1] + fu[2] * fu[2])
        uq = fu[0] * fq[0] + fu[1] * fq[1] + fu[2] * fq[2]
        parts = (
            half * full_sum(rz),
            half * full_sum(zz) + full_sum(z_square),
            half * full_sum(uq),
            half * full_sum(uu) + full_sum(u_square),
        )
        row = jnp.zeros((1, LANES), F32)
        for n, part in enumerate(parts):
            row = jnp.where(lane == n, part, row)

        def reduce_over(row, send_ref, recv_ref, s_sem, r_sem, count, me, peer):
            send_ref[p] = row

            def start(j, _):
                blk, rep = peer(j)
                copy(send_ref.at[p], recv_ref.at[p, me], s_sem.at[p, j], r_sem.at[p, me], blk, rep).start()
                return 0

            lax.fori_loop(1, count, start, 0)
            recv_ref[p, me] = row

            def wait(j, _):
                other = lax.rem(me + j, count)
                copy(send_ref.at[p], recv_ref.at[p, other], s_sem.at[p, j], r_sem.at[p, other], b, r).wait_recv()
                return 0

            lax.fori_loop(1, count, wait, 0)
            total = recv_ref[p, 0]
            for n in range(1, count):
                total = total + recv_ref[p, n]
            return total

        row = reduce_over(
            row, g1send, g1recv, s_g1, r_g1, GROUP, low, lambda j: (inner_peer(j), r)
        )
        row = reduce_over(row, g2send, g2recv, s_g2, r_g2, wide, mine2, outer_peer)

        def scalar(n):
            return jnp.sum(jnp.where(lane == n, row, 0.0), axis=1, keepdims=True)

        rz, zq, uq, uw = scalar(0), scalar(1), scalar(2), scalar(3)
        alpha = rz / zq
        norm_next = rz - 2.0 * alpha * zq + alpha * alpha * uq
        beta = norm_next / rz
        grown = 1.0 + beta
        along = grown * grown * zq - 2.0 * alpha * grown * uq + alpha * alpha * uw
        alpha_two = norm_next / along
        of_z = alpha + alpha_two * grown
        of_u = -alpha * alpha_two
        for c in range(3):
            est[c] = est[c] + of_z * fz[c] + of_u * fu[c]
        if p + 1 < PASSES:

            def new_misfit(k, _):
                for side in range(2):
                    for c in range(3):
                        mis[side, k, c] = (
                            mis[side, k, c] - of_z * chz[side, k, c] - of_u * chu[side, k, c]
                        )
                return 0

            lax.fori_loop(0, pairs, new_misfit, 0)

    for k in range(pairs):
        for t in range(tiles):
            weights_out[0, k : k + 1, t * LANES : (t + 1) * LANES] = wout[k, t : t + 1]
    for h in range(HI):
        at = slice(h * lo_count, (h + 1) * lo_count)
        for c in range(3):
            est_out[c : c + 1, at] = est[c, h : h + 1]

    def drain_init(k, _):
        send_init(k).wait_send()
        send_mis(k).wait_send()
        send_halo(k).wait_send()
        for x in range(2 * PASSES):
            send_ahead(x, k).wait_send()
            send_back(x, k).wait_send()
        return 0

    lax.fori_loop(1, pairs, drain_init, 0)
    for p in range(PASSES):
        copy(bsend.at[p], brecv.at[p], s_b.at[p], r_b.at[p], b, 1 - r).wait_send()
        copy(dsend.at[p], drecv.at[p], s_d.at[p], r_d.at[p], b, 1 - r).wait_send()
        for j in range(1, GROUP):
            copy(g1send.at[p], g1recv.at[p, 0], s_g1.at[p, j], r_g1.at[p, 0], b, r).wait_send()
        for j in range(1, wide):
            copy(g2send.at[p], g2recv.at[p, 0], s_g2.at[p, j], r_g2.at[p, 0], b, r).wait_send()


def on_device(
    n_blk,
    n_rep,
    measured,
    rot_vector,
    confidence,
    first_local,
    second_local,
    edge_counts,
    start_angles,
    anchor,
):
    pairs, slots = first_local.shape[1], first_local.shape[2]
    cams = start_angles.shape[1]
    tiles = slots // LANES
    lo = cams // HI
    wide = (n_blk // GROUP) * n_rep
    vmem = pltpu.VMEM
    sem = pltpu.SemaphoreType.DMA

    def edges(*lead):
        return vmem((*lead, tiles, LANES), F32)

    def cameras(*lead):
        return vmem((*lead, HI, lo), F32)

    scratch = [
        vmem((3 * pairs, lo, slots), BF16),
        vmem((3 * pairs, HI, slots), F32),
        vmem((3 * pairs, tiles, LANES), jnp.int32),
        edges(pairs, 9),
        edges(pairs, 3),
        edges(pairs, 3),
        edges(pairs),
        edges(pairs),
        edges(2, pairs, 3),
        edges(2, pairs, 3),
        edges(2, pairs, 3),
        edges(2, pairs, 3),
        edges(pairs, 4),
        edges(pairs, 4),
        edges(pairs, 3),
        edges(pairs, 3),
        cameras(3),
        cameras(pairs, 3),
        cameras(),
        cameras(6),
        cameras(3),
        cameras(3),
        cameras(3),
        cameras(3),
        cameras(PASSES, 9),
        cameras(PASSES, 9),
        cameras(PASSES, 3),
        cameras(PASSES, 3),
        edges(2 * PASSES, 2, pairs, 3),
        edges(2 * PASSES, 2, pairs, 3),
        vmem((PASSES, 1, LANES), F32),
        vmem((PASSES, GROUP, 1, LANES), F32),
        vmem((PASSES, 1, LANES), F32),
        vmem((PASSES, wide, 1, LANES), F32),
        vmem((2, 144, slots), BF16),
        sem((3, pairs)),
        sem((3, pairs)),
        sem((PASSES,)),
        sem((PASSES,)),
        sem((PASSES,)),
        sem((PASSES,)),
        sem((2 * PASSES, 2, pairs)),
        sem((2 * PASSES, 2, pairs)),
        sem((PASSES, GROUP)),
        sem((PASSES, GROUP)),
        sem((PASSES, wide)),
        sem((PASSES, wide)),
    ]
    whole = pl.BlockSpec(memory_space=pltpu.VMEM)
    return pl.pallas_call(
        functools.partial(kernel, n_blk, n_rep),
        out_shape=(
            jax.ShapeDtypeStruct((3, cams), F32),
            jax.ShapeDtypeStruct((1, pairs, slots), F32),
        ),
        in_specs=[whole] * 8,
        out_specs=(whole, whole),
        scratch_shapes=scratch,
        compiler_params=pltpu.CompilerParams(
            collective_id=0, has_side_effects=True, vmem_limit_bytes=60 * 1024 * 1024
        ),
    )(
        measured,
        rot_vector,
        confidence,
        first_local,
        second_local,
        edge_counts,
        start_angles,
        anchor.reshape(1, -1),
    )


def solution(mesh):
    return jax.shard_map(
        functools.partial(on_device, mesh.shape["blk"], mesh.shape["rep"]),
        mesh=mesh,
        in_specs=(
            P(None, "blk", None, "rep"),
            P(None, "blk", None, "rep"),
            P(None, "blk", None, "rep"),
            P("blk", None, "rep"),
            P("blk", None, "rep"),
            P("blk", None, "rep"),
            P(None, "blk"),
            P("blk"),
        ),
        out_specs=(P(None, "blk"), P("blk", None, "rep")),
        check_vma=False,
    )
```

```python
import functools

import jax
import jax.numpy as jnp
from jax import lax
from jax.experimental import pallas as pl
from jax.experimental.pallas import tpu as pltpu
from jax.sharding import PartitionSpec as P

PASSES = 2
SOFTEN = 0.05
MESH = pl.DeviceIdType.MESH
LANES = 128
HI = 8
GROUP = 8
PAIRS = ((0, 0), (0, 1), (0, 2), (1, 1), (1, 2), (2, 2))
F32 = jnp.float32
BF16 = jnp.bfloat16


UG = 8
US = 4
UB = 4


def loop(first, last, body, init, unroll):
    if unroll < last - first:
        return lax.fori_loop(first, last, body, init, unroll=unroll)
    for i in range(first, last):
        init = body(i, init)
    return init


def dot_nn(a, b):
    return lax.dot_general(a, b, (((1,), (0,)), ((), ())), preferred_element_type=F32)


def dot_nt(a, b):
    return lax.dot_general(a, b, (((1,), (1,)), ((), ())), preferred_element_type=F32)


def pieces_of(value, count):
    found = []
    for _ in range(count - 1):
        found.append(value.astype(BF16).astype(F32))
        value = value - found[-1]
    return found + [value]


def kernel(
    n_blk,
    n_rep,
    measured_in,
    rot_in,
    conf_in,
    first_in,
    second_in,
    counts_in,
    start_in,
    anchor_in,
    est_out,
    weights_out,
    hot,
    himask,
    idx,
    rotm,
    meas,
    conf,
    live,
    wout,
    mis,
    wconf,
    chz,
    chu,
    send1,
    recv1,
    send2,
    recv2,
    est,
    halo,
    anc,
    inv,
    fz,
    fu,
    fr,
    fq,
    bsend,
    brecv,
    dsend,
    drecv,
    xsend,
    xrecv,
    g1send,
    g1recv,
    g2send,
    g2recv,
    lhs,
    s_init,
    r_init,
    s_b,
    r_b,
    s_d,
    r_d,
    s_x,
    r_x,
    s_g1,
    r_g1,
    s_g2,
    r_g2,
    measured_ref,
    rot_ref,
    conf_ref,
    first_ref,
    second_ref,
    counts_ref,
    start_ref,
    anchor_ref,
    s_in,
):
    pairs = idx.shape[0] // 3
    tiles = idx.shape[1]
    lo_count = est.shape[2]
    outer = n_blk // GROUP
    wide = outer * n_rep
    b = lax.axis_index("blk")
    r = lax.axis_index("rep")
    low = lax.rem(b, GROUP)
    high = b // GROUP
    mine2 = high * n_rep + r

    def ahead(k):
        return lax.rem(b + k, n_blk)

    def behind(k):
        return lax.rem(b + n_blk - k, n_blk)

    def copy(src, dst, send, recv, blk, rep):
        return pltpu.make_async_remote_copy(
            src_ref=src,
            dst_ref=dst,
            send_sem=send,
            recv_sem=recv,
            device_id={"blk": blk, "rep": rep},
            device_id_type=MESH,
        )

    pending = []

    def drain():
        while pending:
            pending.pop(0)()

    def later(first, last, wait):
        def loop():
            def step(k, _):
                wait(k)
                return 0

            lax.fori_loop(first, last, step, 0)

        pending.append(loop)

    barrier = pltpu.get_barrier_semaphore()

    def greet(blk, rep):
        pl.semaphore_signal(barrier, inc=1, device_id={"blk": blk, "rep": rep}, device_id_type=MESH)

    def greet_pairs(k, _):
        greet(ahead(k), r)
        greet(behind(k), r)
        return 0

    lax.fori_loop(1, pairs, greet_pairs, 0)
    greet(b, 1 - r)

    def inner_peer(j):
        return high * GROUP + lax.rem(low + j, GROUP)

    def outer_peer(j):
        other = lax.rem(mine2 + j, wide)
        return (other // n_rep) * GROUP + low, lax.rem(other, n_rep)

    def greet_inner(j, _):
        greet(inner_peer(j), r)
        return 0

    def greet_outer(j, _):
        blk, rep = outer_peer(j)
        greet(blk, rep)
        return 0

    lax.fori_loop(1, GROUP, greet_inner, 0)
    lax.fori_loop(1, wide, greet_outer, 0)

    loads = [
        pltpu.make_async_copy(src, dst, s_in.at[n])
        for n, (src, dst) in enumerate(
            (
                (start_in, start_ref),
                (second_in, second_ref),
                (conf_in, conf_ref),
                (counts_in, counts_ref),
                (first_in, first_ref),
                (rot_in, rot_ref),
                (measured_in, measured_ref),
                (anchor_in, anchor_ref),
            )
        )
    ]
    for load in loads:
        load.start()
    for load in loads:
        load.wait()
    slot = lax.broadcasted_iota(jnp.int32, (tiles, LANES), 0) * LANES
    slot = slot + lax.broadcasted_iota(jnp.int32, (tiles, LANES), 1)
    for k in range(pairs):
        live[k] = jnp.where(slot < counts_ref[0:1, k : k + 1], 1.0, 0.0).astype(F32)
        for t in range(tiles):
            at = slice(t * LANES, (t + 1) * LANES)
            idx[k, t : t + 1] = first_ref[0, k : k + 1, at]
            idx[2 * pairs + k, t : t + 1] = second_ref[0, k : k + 1, at]
            for c in range(3):
                conf[k, c, t : t + 1] = conf_ref[c, 0, k : k + 1, at]
                meas[k, c, t : t + 1] = measured_ref[c, 0, k : k + 1, at]
                rotm[k, c, t : t + 1] = rot_ref[c, 0, k : k + 1, at]
    for h in range(HI):
        at = slice(h * lo_count, (h + 1) * lo_count)
        anc[h : h + 1] = anchor_ref[0:1, at]
        for c in range(3):
            est[c, h : h + 1] = start_ref[c : c + 1, at]

    def stage1(k, _):
        for c in range(3):
            conf[k, c] = conf[k, c] * live[k]
            send1[k, c] = conf[k, c]
        send1[k, 3] = idx[2 * pairs + k].astype(F32)
        return 0

    lax.fori_loop(0, pairs, stage1, 0)
    halo[0] = est[...]

    pl.semaphore_wait(barrier, 2 * (pairs - 1) + 1 + (GROUP - 1) + (wide - 1))

    def send_init(k):
        return copy(send1.at[k], recv1.at[k], s_init.at[0, k], r_init.at[0, k], ahead(k), r)

    def send_mis(k):
        return copy(send2.at[k], recv2.at[k], s_init.at[1, k], r_init.at[1, k], ahead(k), r)

    def send_halo(k):
        return copy(halo.at[0], halo.at[k], s_init.at[2, k], r_init.at[2, k], behind(k), r)

    def start_init(k, _):
        send_init(k).start()
        send_halo(k).start()
        return 0

    lax.fori_loop(1, pairs, start_init, 0)
    later(1, pairs, lambda k: (send_init(k).wait_send(), send_halo(k).wait_send()))
    recv1[0] = send1[0]

    def rotations(k, _):
        v = [rotm[k, c] for c in range(3)]
        squared = v[0] * v[0] + v[1] * v[1] + v[2] * v[2]
        factor = 2.0 / (1.0 + squared)
        zero = jnp.zeros_like(squared)
        skew = ((zero, -v[2], v[1]), (v[2], zero, -v[0]), (-v[1], v[0], zero))
        for i in range(3):
            for j in range(3):
                term = skew[i][j] + v[i] * v[j]
                if i == j:
                    rotm[k, 3 * i + j] = 1.0 + factor * (term - squared)
                else:
                    rotm[k, 3 * i + j] = factor * term
        return 0

    lax.fori_loop(0, pairs, rotations, 0)

    def build(g):
        for t in range(tiles):
            where = idx[g, t : t + 1]
            low_part = lax.rem(where, lo_count)
            high_part = where // lo_count
            at = slice(t * LANES, (t + 1) * LANES)
            himask[g, :, at] = jnp.where(
                lax.broadcasted_iota(jnp.int32, (HI, LANES), 0) == high_part, 1.0, 0.0
            ).astype(F32)
            hot[g, :, at] = jnp.where(
                lax.broadcasted_iota(jnp.int32, (lo_count, LANES), 0) == low_part, 1.0, 0.0
            ).astype(BF16)

    def build_near(k, _):
        build(k)
        return 0

    def build_second(k, _):
        build(2 * pairs + k)
        return 0

    def table_of(field, count):
        rows = []
        for c in range(3):
            rows.extend(pieces_of(field[c], count))
        return jnp.concatenate(rows, axis=0).astype(BF16)

    def gather(table, g):
        full = dot_nn(table, hot[g])
        mask = himask[g]
        count = table.shape[0] // (3 * HI)
        found = []
        for c in range(3):
            part = full[HI * count * c : HI * count * c + HI]
            for n in range(1, count):
                part = part + full[HI * (count * c + n) : HI * (count * c + n + 1)]
            part = part * mask
            row = jnp.sum(part, axis=0, keepdims=True)
            found.append(
                jnp.concatenate([row[:, t * LANES : (t + 1) * LANES] for t in range(tiles)], axis=0)
            )
        return found

    def rotate(k, vec):
        return [
            rotm[k, 3 * i] * vec[0] + rotm[k, 3 * i + 1] * vec[1] + rotm[k, 3 * i + 2] * vec[2]
            for i in range(3)
        ]

    def rotate_back(k, vec):
        return [
            rotm[k, i] * vec[0] + rotm[k, 3 + i] * vec[1] + rotm[k, 6 + i] * vec[2]
            for i in range(3)
        ]

    loop(0, pairs, build_near, 0, UB)
    table = table_of(est, 3)

    def near_start(i, _):
        k = (i + 1) % pairs
        turned = rotate(k, gather(table, k))
        for c in range(3):
            send2[k, c] = meas[k, c] + turned[c]

        @pl.when(k != 0)
        def _():
            send_mis(k).start()

        return 0

    loop(0, pairs, near_start, 0, UG)
    later(1, pairs, lambda k: send_mis(k).wait_send())
    recv2[0] = send2[0]

    loop(0, pairs, build_second, 0, UB)

    def wait_halo(k, _):
        copy(halo.at[0], halo.at[k], s_init.at[2, k], r_init.at[2, k], b, r).wait_recv()
        return 0

    lax.fori_loop(1, pairs, wait_halo, 0)

    def own_misfit(k, _):
        there = gather(table_of(halo.at[k], 3), 2 * pairs + k)
        for c in range(3):
            mis[0, k, c] = send2[k, c] - there[c]
        return 0

    loop(0, pairs, own_misfit, 0, UG)

    def wait_init(k, _):
        copy(send1.at[k], recv1.at[k], s_init.at[0, k], r_init.at[0, k], b, r).wait_recv()
        return 0

    lax.fori_loop(1, pairs, wait_init, 0)

    def build_far(k, _):
        idx[pairs + k] = recv1[k, 3].astype(jnp.int32)
        build(pairs + k)
        return 0

    loop(0, pairs, build_far, 0, UB)

    def wait_mis(k, _):
        copy(send2.at[k], recv2.at[k], s_init.at[1, k], r_init.at[1, k], b, r).wait_recv()
        return 0

    lax.fori_loop(1, pairs, wait_mis, 0)

    def far_misfit(k, _):
        there = gather(table, pairs + k)
        for c in range(3):
            mis[1, k, c] = recv2[k, c] - there[c]
        return 0

    loop(0, pairs, far_misfit, 0, UG)

    def put(slot, at_row, terms, g):
        for n, term in enumerate(terms):
            head, tail = pieces_of(term, 2)
            for t in range(tiles):
                at = slice(t * LANES, (t + 1) * LANES)
                mask = himask[g, :, at]
                both = jnp.concatenate([head[t : t + 1] * mask, tail[t : t + 1] * mask], axis=0)
                lhs[slot, at_row + 16 * n : at_row + 16 * n + 16, at] = both.astype(BF16)

    def summed(totals, channel):
        return totals[16 * channel : 16 * channel + 8] + totals[16 * channel + 8 : 16 * channel + 16]

    def full_sum(value):
        return jnp.sum(jnp.sum(value, axis=0, keepdims=True), axis=1, keepdims=True)

    def invert(vec_ref, out_ref):
        for i in range(3):
            look = ((0, 1, 2), (1, 3, 4), (2, 4, 5))[i]
            out_ref[i] = (
                inv[look[0]] * vec_ref[0] + inv[look[1]] * vec_ref[1] + inv[look[2]] * vec_ref[2]
            )

    def exchange_start(x, table):
        def step(i, _):
            k = (i + 1) % pairs
            turned = rotate(k, gather(table, k))
            there = gather(table, pairs + k)
            for c in range(3):
                xsend[x, 0, k, c] = turned[c]
                xsend[x, 1, k, c] = there[c]

            @pl.when(k != 0)
            def _():
                send_back(x, k).start()
                send_ahead(x, k).start()

            return 0

        loop(0, pairs, step, 0, UG)
        later(1, pairs, lambda k: (send_back(x, k).wait_send(), send_ahead(x, k).wait_send()))
        xrecv[x, 0, 0] = xsend[x, 0, 0]
        xrecv[x, 1, 0] = xsend[x, 1, 0]

    def send_ahead(x, k):
        return copy(xsend.at[x, 0, k], xrecv.at[x, 0, k], s_x.at[x, 0, k], r_x.at[x, 0, k], ahead(k), r)

    def send_back(x, k):
        return copy(xsend.at[x, 1, k], xrecv.at[x, 1, k], s_x.at[x, 1, k], r_x.at[x, 1, k], behind(k), r)

    def to_twin(src, dst, send, recv, p):
        both = copy(src.at[p], dst.at[p], send.at[p], recv.at[p], b, 1 - r)
        both.start()
        pending.append(both.wait_send)
        both.wait_recv()

    def wait_exchange(x, k):
        @pl.when(k != 0)
        def _():
            copy(xsend.at[x, 1, k], xrecv.at[x, 1, k], s_x.at[x, 1, k], r_x.at[x, 1, k], b, r).wait_recv()
            copy(xsend.at[x, 0, k], xrecv.at[x, 0, k], s_x.at[x, 0, k], r_x.at[x, 0, k], b, r).wait_recv()

    lane = lax.broadcasted_iota(jnp.int32, (1, LANES), 1)

    def one_pass(p, _):
        def near_sums(k, totals):
            m = [mis[0, k, c] for c in range(3)]
            cf = [conf[k, c] for c in range(3)]
            squares = cf[0] * m[0] * m[0] + cf[1] * m[1] * m[1] + cf[2] * m[2] * m[2]
            weight = live[k] / jnp.sqrt(squares + SOFTEN * SOFTEN)
            wout[k] = weight
            wc = [weight * cf[c] for c in range(3)]
            for c in range(3):
                wconf[0, k, c] = wc[c]
            back = rotate_back(k, [wc[c] * m[c] for c in range(3)])
            rot = [[rotm[k, 3 * i + j] for j in range(3)] for i in range(3)]
            terms = [-value for value in back]
            for f, s in PAIRS:
                terms.append(
                    rot[0][f] * wc[0] * rot[0][s]
                    + rot[1][f] * wc[1] * rot[1][s]
                    + rot[2][f] * wc[2] * rot[2][s]
                )
            put(k, 0, terms, k)
            return totals + dot_nt(lhs[k], hot[k])

        def far_sums(k, totals):
            m = [mis[1, k, c] for c in range(3)]
            cf = [recv1[k, c] for c in range(3)]
            squares = cf[0] * m[0] * m[0] + cf[1] * m[1] * m[1] + cf[2] * m[2] * m[2]
            weight = 1.0 / jnp.sqrt(squares + SOFTEN * SOFTEN)
            wc = [weight * cf[c] for c in range(3)]
            for c in range(3):
                wconf[1, k, c] = wc[c]
            put(pairs + k, 0, [wc[c] * m[c] for c in range(3)] + wc, pairs + k)
            return totals + dot_nt(lhs[pairs + k, 0:96], hot[pairs + k])

        near = loop(0, pairs, near_sums, jnp.zeros((144, lo_count), F32), US)
        far = loop(0, pairs, far_sums, jnp.zeros((96, lo_count), F32), US)
        for n in range(9):
            total = summed(near, n)
            spot = {0: 0, 1: 1, 2: 2, 3: 3, 6: 4, 8: 5}.get(n)
            if spot is not None:
                total = total + summed(far, spot)
            bsend[p, n] = total
        to_twin(bsend, brecv, s_b, r_b, p)
        anchor = anc[...]
        for c in range(3):
            fr[c] = bsend[p, c] + brecv[p, c] - anchor * est[c]
        blocks = []
        for n, (f, s) in enumerate(PAIRS):
            block = bsend[p, 3 + n] + brecv[p, 3 + n]
            blocks.append(block + anchor if f == s else block)
        adjugate = [
            blocks[3] * blocks[5] - blocks[4] * blocks[4],
            blocks[2] * blocks[4] - blocks[1] * blocks[5],
            blocks[1] * blocks[4] - blocks[2] * blocks[3],
            blocks[0] * blocks[5] - blocks[2] * blocks[2],
            blocks[1] * blocks[2] - blocks[0] * blocks[4],
            blocks[0] * blocks[3] - blocks[1] * blocks[1],
        ]
        determinant = blocks[0] * adjugate[0] + blocks[1] * adjugate[1] + blocks[2] * adjugate[2]
        for n in range(6):
            inv[n] = adjugate[n] / determinant
        invert(fr, fz)

        x = 2 * p
        exchange_start(x, table_of(fz, 2))

        def product_near(k, totals):
            wait_exchange(x, k)
            change = [xrecv[x, 1, k, c] - xsend[x, 0, k, c] for c in range(3)]
            pushed = []
            square = totals[1]
            for c in range(3):
                chz[0, k, c] = change[c]
                pushed.append(wconf[0, k, c] * change[c])
                square = square + pushed[c] * change[c]
            put(k, 0, [-value for value in rotate_back(k, pushed)], k)
            return totals[0] + dot_nt(lhs[k, 0:48], hot[k]), square

        def product_far(k, totals):
            change = [xsend[x, 1, k, c] - xrecv[x, 0, k, c] for c in range(3)]
            pushed = []
            for c in range(3):
                chz[1, k, c] = change[c]
                pushed.append(wconf[1, k, c] * change[c])
            put(pairs + k, 0, pushed, pairs + k)
            return totals + dot_nt(lhs[pairs + k, 0:48], hot[pairs + k])

        zero_row = jnp.zeros((tiles, LANES), F32)
        totals, z_square = loop(
            0, pairs, product_near, (jnp.zeros((48, lo_count), F32), zero_row), US
        )
        totals = loop(0, pairs, product_far, totals, US)
        for c in range(3):
            dsend[p, c] = summed(totals, c)
        to_twin(dsend, drecv, s_d, r_d, p)
        for c in range(3):
            fq[c] = dsend[p, c] + drecv[p, c] + anchor * fz[c]
        invert(fq, fu)

        y = 2 * p + 1
        exchange_start(y, table_of(fu, 2))

        def change_u(k, square):
            wait_exchange(y, k)
            for c in range(3):
                change = xrecv[y, 1, k, c] - xsend[y, 0, k, c]
                chu[0, k, c] = change
                square = square + wconf[0, k, c] * change * change
                chu[1, k, c] = xsend[y, 1, k, c] - xrecv[y, 0, k, c]
            return square

        u_square = lax.fori_loop(0, pairs, change_u, zero_row)

        half = 1.0 / n_rep
        rz = fr[0] * fz[0] + fr[1] * fz[1] + fr[2] * fz[2]
        zz = anchor * (fz[0] * fz[0] + fz[1] * fz[1] + fz[2] * fz[2])
        uu = anchor * (fu[0] * fu[0] + fu[1] * fu[1] + fu[2] * fu[2])
        uq = fu[0] * fq[0] + fu[1] * fq[1] + fu[2] * fq[2]
        parts = (
            half * full_sum(rz),
            half * full_sum(zz) + full_sum(z_square),
            half * full_sum(uq),
            half * full_sum(uu) + full_sum(u_square),
        )
        row = jnp.zeros((1, LANES), F32)
        for n, part in enumerate(parts):
            row = jnp.where(lane == n, part, row)

        def reduce_over(row, send_ref, recv_ref, s_sem, r_sem, count, me, peer):
            send_ref[p] = row

            def start(j, _):
                blk, rep = peer(j)
                copy(send_ref.at[p], recv_ref.at[p, me], s_sem.at[p, j], r_sem.at[p, me], blk, rep).start()
                return 0

            lax.fori_loop(1, count, start, 0)
            drain()
            later(
                1,
                count,
                lambda j: copy(
                    send_ref.at[p], recv_ref.at[p, me], s_sem.at[p, j], r_sem.at[p, me], b, r
                ).wait_send(),
            )
            recv_ref[p, me] = row

            def wait(j, _):
                other = lax.rem(me + j, count)
                copy(send_ref.at[p], recv_ref.at[p, other], s_sem.at[p, j], r_sem.at[p, other], b, r).wait_recv()
                return 0

            lax.fori_loop(1, count, wait, 0)
            total = recv_ref[p, 0]
            for n in range(1, count):
                total = total + recv_ref[p, n]
            return total

        row = reduce_over(
            row, g1send, g1recv, s_g1, r_g1, GROUP, low, lambda j: (inner_peer(j), r)
        )
        row = reduce_over(row, g2send, g2recv, s_g2, r_g2, wide, mine2, outer_peer)

        def scalar(n):
            return jnp.sum(jnp.where(lane == n, row, 0.0), axis=1, keepdims=True)

        rz, zq, uq, uw = scalar(0), scalar(1), scalar(2), scalar(3)
        alpha = rz / zq
        norm_next = rz - 2.0 * alpha * zq + alpha * alpha * uq
        beta = norm_next / rz
        grown = 1.0 + beta
        along = grown * grown * zq - 2.0 * alpha * grown * uq + alpha * alpha * uw
        alpha_two = norm_next / along
        of_z = alpha + alpha_two * grown
        of_u = -alpha * alpha_two
        for c in range(3):
            est[c] = est[c] + of_z * fz[c] + of_u * fu[c]
        @pl.when(p + 1 < PASSES)
        def _():
            def new_misfit(k, _):
                for side in range(2):
                    for c in range(3):
                        mis[side, k, c] = (
                            mis[side, k, c] - of_z * chz[side, k, c] - of_u * chu[side, k, c]
                        )
                return 0

            lax.fori_loop(0, pairs, new_misfit, 0)

        drain()
        return 0

    drain()
    lax.fori_loop(0, PASSES, one_pass, 0)

    for k in range(pairs):
        for t in range(tiles):
            weights_out[0, k : k + 1, t * LANES : (t + 1) * LANES] = wout[k, t : t + 1]
    for h in range(HI):
        at = slice(h * lo_count, (h + 1) * lo_count)
        for c in range(3):
            est_out[c : c + 1, at] = est[c, h : h + 1]


def on_device(
    n_blk,
    n_rep,
    measured,
    rot_vector,
    confidence,
    first_local,
    second_local,
    edge_counts,
    start_angles,
    anchor,
):
    pairs, slots = first_local.shape[1], first_local.shape[2]
    cams = start_angles.shape[1]
    tiles = slots // LANES
    lo = cams // HI
    wide = (n_blk // GROUP) * n_rep
    vmem = pltpu.VMEM
    sem = pltpu.SemaphoreType.DMA

    def edges(*lead):
        return vmem((*lead, tiles, LANES), F32)

    def cameras(*lead):
        return vmem((*lead, HI, lo), F32)

    scratch = [
        vmem((3 * pairs, lo, slots), BF16),
        vmem((3 * pairs, HI, slots), F32),
        vmem((3 * pairs, tiles, LANES), jnp.int32),
        edges(pairs, 9),
        edges(pairs, 3),
        edges(pairs, 3),
        edges(pairs),
        edges(pairs),
        edges(2, pairs, 3),
        edges(2, pairs, 3),
        edges(2, pairs, 3),
        edges(2, pairs, 3),
        edges(pairs, 4),
        edges(pairs, 4),
        edges(pairs, 3),
        edges(pairs, 3),
        cameras(3),
        cameras(pairs, 3),
        cameras(),
        cameras(6),
        cameras(3),
        cameras(3),
        cameras(3),
        cameras(3),
        cameras(PASSES, 9),
        cameras(PASSES, 9),
        cameras(PASSES, 3),
        cameras(PASSES, 3),
        edges(2 * PASSES, 2, pairs, 3),
        edges(2 * PASSES, 2, pairs, 3),
        vmem((PASSES, 1, LANES), F32),
        vmem((PASSES, GROUP, 1, LANES), F32),
        vmem((PASSES, 1, LANES), F32),
        vmem((PASSES, wide, 1, LANES), F32),
        vmem((2 * pairs, 144, slots), BF16),
        sem((3, pairs)),
        sem((3, pairs)),
        sem((PASSES,)),
        sem((PASSES,)),
        sem((PASSES,)),
        sem((PASSES,)),
        sem((2 * PASSES, 2, pairs)),
        sem((2 * PASSES, 2, pairs)),
        sem((PASSES, GROUP)),
        sem((PASSES, GROUP)),
        sem((PASSES, wide)),
        sem((PASSES, wide)),
        vmem(measured.shape, F32),
        vmem(rot_vector.shape, F32),
        vmem(confidence.shape, F32),
        vmem(first_local.shape, jnp.int32),
        vmem(second_local.shape, jnp.int32),
        vmem((1, pairs), jnp.int32),
        vmem(start_angles.shape, F32),
        vmem((1, cams), F32),
        sem((8,)),
    ]
    whole = pl.BlockSpec(memory_space=pltpu.VMEM)
    return pl.pallas_call(
        functools.partial(kernel, n_blk, n_rep),
        out_shape=(
            pltpu.VMEM((3, cams), F32),
            pltpu.VMEM((1, pairs, slots), F32),
        ),
        in_specs=[pl.BlockSpec(memory_space=pl.ANY)] * 8,
        out_specs=(whole, whole),
        scratch_shapes=scratch,
        compiler_params=pltpu.CompilerParams(
            collective_id=0, has_side_effects=True, vmem_limit_bytes=60 * 1024 * 1024
        ),
    )(
        measured,
        rot_vector,
        confidence,
        first_local,
        second_local,
        edge_counts.reshape(1, -1),
        start_angles,
        anchor.reshape(1, -1),
    )


def solution(mesh):
    return jax.shard_map(
        functools.partial(on_device, mesh.shape["blk"], mesh.shape["rep"]),
        mesh=mesh,
        in_specs=(
            P(None, "blk", None, "rep"),
            P(None, "blk", None, "rep"),
            P(None, "blk", None, "rep"),
            P("blk", None, "rep"),
            P("blk", None, "rep"),
            P("blk", None, "rep"),
            P(None, "blk"),
            P("blk"),
        ),
        out_specs=(P(None, "blk"), P("blk", None, "rep")),
        check_vma=False,
    )
```

```python
import functools

import jax
import jax.numpy as jnp
from jax import lax
from jax.experimental import pallas as pl
from jax.experimental.pallas import tpu as pltpu
from jax.sharding import PartitionSpec as P

PASSES = 2
SOFTEN = 0.05
MESH = pl.DeviceIdType.MESH
LANES = 128
HI = 16
GROUP = 8
DIAGONAL = ((0, 0), (1, 1), (2, 2))
OTHERS = ((0, 1), (0, 2), (1, 2))
F32 = jnp.float32
BF16 = jnp.bfloat16


UG = 8
US = 4
UB = 4


def loop(first, last, body, init, unroll):
    if unroll < last - first:
        return lax.fori_loop(first, last, body, init, unroll=unroll)
    for i in range(first, last):
        init = body(i, init)
    return init


def dot_nn(a, b):
    return lax.dot_general(a, b, (((1,), (0,)), ((), ())), preferred_element_type=F32)


def dot_nt(a, b):
    return lax.dot_general(a, b, (((1,), (1,)), ((), ())), preferred_element_type=F32)


def pieces_of(value, count):
    found = []
    for _ in range(count - 1):
        found.append(value.astype(BF16).astype(F32))
        value = value - found[-1]
    return found + [value]


def kernel(
    n_blk,
    n_rep,
    measured_in,
    rot_in,
    conf_in,
    first_in,
    second_in,
    counts_in,
    start_in,
    anchor_in,
    est_out,
    weights_out,
    hot,
    himask,
    idx,
    rotm,
    meas,
    conf,
    live,
    wout,
    mis,
    wconf,
    chz,
    chu,
    send1,
    recv1,
    send2,
    recv2,
    est,
    halo,
    anc,
    inv,
    fz,
    fu,
    fr,
    fq,
    bsend,
    brecv,
    dsend,
    drecv,
    xsend,
    xrecv,
    g1send,
    g1recv,
    g2send,
    g2recv,
    lhs,
    s_init,
    r_init,
    s_b,
    r_b,
    s_d,
    r_d,
    s_x,
    r_x,
    s_g1,
    r_g1,
    s_g2,
    r_g2,
    measured_ref,
    rot_ref,
    conf_ref,
    first_ref,
    second_ref,
    counts_ref,
    start_ref,
    anchor_ref,
    s_in,
):
    pairs = idx.shape[0] // 3
    tiles = idx.shape[1]
    rows_of = 2 * HI
    lo_count = est.shape[2]
    outer = n_blk // GROUP
    wide = outer * n_rep
    b = lax.axis_index("blk")
    r = lax.axis_index("rep")
    low = lax.rem(b, GROUP)
    high = b // GROUP
    mine2 = high * n_rep + r

    def ahead(k):
        return lax.rem(b + k, n_blk)

    def behind(k):
        return lax.rem(b + n_blk - k, n_blk)

    def copy(src, dst, send, recv, blk, rep):
        return pltpu.make_async_remote_copy(
            src_ref=src,
            dst_ref=dst,
            send_sem=send,
            recv_sem=recv,
            device_id={"blk": blk, "rep": rep},
            device_id_type=MESH,
        )

    pending = []

    def drain():
        while pending:
            pending.pop(0)()

    def later(first, last, wait):
        def loop():
            def step(k, _):
                wait(k)
                return 0

            lax.fori_loop(first, last, step, 0)

        pending.append(loop)

    barrier = pltpu.get_barrier_semaphore()

    def greet(blk, rep):
        pl.semaphore_signal(barrier, inc=1, device_id={"blk": blk, "rep": rep}, device_id_type=MESH)

    ahead_of = [ahead(k) for k in range(pairs)]
    behind_of = [behind(k) for k in range(pairs)]
    for k in range(1, pairs):
        greet(ahead_of[k], r)
        greet(behind_of[k], r)
    greet(b, 1 - r)

    def inner_peer(j):
        return high * GROUP + lax.rem(low + j, GROUP)

    def outer_peer(j):
        other = lax.rem(mine2 + j, wide)
        return (other // n_rep) * GROUP + low, lax.rem(other, n_rep)

    inner_of = [(inner_peer(j), r) for j in range(GROUP)]
    outer_of = [outer_peer(j) for j in range(wide)]
    for blk, rep in inner_of[1:] + outer_of[1:]:
        greet(blk, rep)

    loads = [
        pltpu.make_async_copy(src, dst, s_in.at[n])
        for n, (src, dst) in enumerate(
            (
                (start_in, start_ref),
                (second_in, second_ref),
                (conf_in, conf_ref),
                (counts_in, counts_ref),
                (first_in, first_ref),
                (rot_in, rot_ref),
                (measured_in, measured_ref),
                (anchor_in, anchor_ref),
            )
        )
    ]
    for load in loads:
        load.start()
    for load in loads:
        load.wait()
    slot = lax.broadcasted_iota(jnp.int32, (tiles, LANES), 0) * LANES
    slot = slot + lax.broadcasted_iota(jnp.int32, (tiles, LANES), 1)
    for k in range(pairs):
        live[k] = jnp.where(slot < counts_ref[0:1, k : k + 1], 1.0, 0.0).astype(F32)
        for t in range(tiles):
            at = slice(t * LANES, (t + 1) * LANES)
            idx[k, t : t + 1] = first_ref[0, k : k + 1, at]
            idx[2 * pairs + k, t : t + 1] = second_ref[0, k : k + 1, at]
            for c in range(3):
                conf[k, c, t : t + 1] = conf_ref[c, 0, k : k + 1, at]
                meas[k, c, t : t + 1] = measured_ref[c, 0, k : k + 1, at]
                rotm[k, c, t : t + 1] = rot_ref[c, 0, k : k + 1, at]
    for h in range(HI):
        at = slice(h * lo_count, (h + 1) * lo_count)
        anc[h : h + 1] = anchor_ref[0:1, at]
        for c in range(3):
            est[c, h : h + 1] = start_ref[c : c + 1, at]

    def stage1(k, _):
        for c in range(3):
            conf[k, c] = conf[k, c] * live[k]
            send1[k, c] = conf[k, c]
        send1[k, 3] = idx[2 * pairs + k].astype(F32)
        return 0

    lax.fori_loop(0, pairs, stage1, 0)
    halo[0] = est[...]

    def send_init(k, blk):
        return copy(send1.at[k], recv1.at[k], s_init.at[0, k], r_init.at[0, k], blk, r)

    def send_mis(k, blk):
        return copy(send2.at[k], recv2.at[k], s_init.at[1, k], r_init.at[1, k], blk, r)

    def send_halo(k, blk):
        return copy(halo.at[0], halo.at[k], s_init.at[2, k], r_init.at[2, k], blk, r)

    pl.semaphore_wait(barrier, 2 * (pairs - 1) + 1 + (GROUP - 1) + (wide - 1))
    for k in range(1, pairs):
        send_halo(k, behind_of[k]).start()
        send_init(k, ahead_of[k]).start()

    def rotations(k, _):
        v = [rotm[k, c] for c in range(3)]
        squared = v[0] * v[0] + v[1] * v[1] + v[2] * v[2]
        factor = 2.0 / (1.0 + squared)
        zero = jnp.zeros_like(squared)
        skew = ((zero, -v[2], v[1]), (v[2], zero, -v[0]), (-v[1], v[0], zero))
        for i in range(3):
            for j in range(3):
                term = skew[i][j] + v[i] * v[j]
                if i == j:
                    rotm[k, 3 * i + j] = 1.0 + factor * (term - squared)
                else:
                    rotm[k, 3 * i + j] = factor * term
        return 0

    lax.fori_loop(0, pairs, rotations, 0)

    def build(g):
        for t in range(tiles):
            where = idx[g, t : t + 1]
            low_part = lax.rem(where, lo_count)
            high_part = where // lo_count
            at = slice(t * LANES, (t + 1) * LANES)
            himask[g, :, at] = jnp.where(
                lax.broadcasted_iota(jnp.int32, (HI, LANES), 0) == high_part, 1.0, 0.0
            ).astype(F32)
            hot[g, :, at] = jnp.where(
                lax.broadcasted_iota(jnp.int32, (lo_count, LANES), 0) == low_part, 1.0, 0.0
            ).astype(BF16)

    def build_near(k, _):
        build(k)
        return 0

    def build_second(k, _):
        build(2 * pairs + k)
        return 0

    def table_of(field, count):
        rows = []
        for c in range(3):
            rows.extend(pieces_of(field[c], count))
        return jnp.concatenate(rows, axis=0).astype(BF16)

    def gather(table, g):
        full = dot_nn(table, hot[g])
        mask = himask[g]
        count = table.shape[0] // (3 * HI)
        found = []
        for c in range(3):
            part = full[HI * count * c : HI * count * c + HI]
            for n in range(1, count):
                part = part + full[HI * (count * c + n) : HI * (count * c + n + 1)]
            part = part * mask
            row = jnp.sum(part, axis=0, keepdims=True)
            found.append(
                jnp.concatenate([row[:, t * LANES : (t + 1) * LANES] for t in range(tiles)], axis=0)
            )
        return found

    def rotate(k, vec):
        return [
            rotm[k, 3 * i] * vec[0] + rotm[k, 3 * i + 1] * vec[1] + rotm[k, 3 * i + 2] * vec[2]
            for i in range(3)
        ]

    def rotate_back(k, vec):
        return [
            rotm[k, i] * vec[0] + rotm[k, 3 + i] * vec[1] + rotm[k, 6 + i] * vec[2]
            for i in range(3)
        ]

    loop(0, pairs, build_near, 0, UB)
    table = table_of(est, 3)

    def near_start(k, _):
        turned = rotate(k, gather(table, k))
        for c in range(3):
            send2[k, c] = meas[k, c] + turned[c]
        if k != 0:
            send_mis(k, ahead_of[k]).start()
        return 0

    loop(0, pairs, near_start, 0, pairs)
    loop(0, pairs, build_second, 0, UB)
    later(
        1,
        pairs,
        lambda k: [send(k, b).wait_send() for send in (send_init, send_mis, send_halo)],
    )
    recv1[0] = send1[0]
    recv2[0] = send2[0]

    for k in range(1, pairs):
        send_init(k, b).wait_recv()

    def build_far(k, _):
        idx[pairs + k] = recv1[k, 3].astype(jnp.int32)
        build(pairs + k)
        return 0

    loop(0, pairs, build_far, 0, UB)

    def far_misfit(k, _):
        there = gather(table, pairs + k)
        for c in range(3):
            mis[1, k, c] = recv2[k, c] - there[c]
        return 0

    for k in range(1, pairs):
        send_mis(k, b).wait_recv()
    loop(0, pairs, far_misfit, 0, UG)
    for k in range(1, pairs):
        send_halo(k, b).wait_recv()

    def own_misfit(k, _):
        there = gather(table_of(halo.at[k], 3), 2 * pairs + k)
        for c in range(3):
            mis[0, k, c] = send2[k, c] - there[c]
        return 0

    loop(0, pairs, own_misfit, 0, UG)

    def put(slot, at_row, terms, g):
        for n, term in enumerate(terms):
            head, tail = pieces_of(term, 2)
            for t in range(tiles):
                at = slice(t * LANES, (t + 1) * LANES)
                mask = himask[g, :, at]
                both = jnp.concatenate([head[t : t + 1] * mask, tail[t : t + 1] * mask], axis=0)
                lhs[slot, at_row + rows_of * n : at_row + rows_of * (n + 1), at] = both.astype(BF16)

    def summed(totals, channel):
        at = rows_of * channel
        return totals[at : at + HI] + totals[at + HI : at + rows_of]

    def full_sum(value):
        return jnp.sum(jnp.sum(value, axis=0, keepdims=True), axis=1, keepdims=True)

    def invert(vec_ref, out_ref):
        for i in range(3):
            look = ((0, 1, 2), (1, 3, 4), (2, 4, 5))[i]
            out_ref[i] = (
                inv[look[0]] * vec_ref[0] + inv[look[1]] * vec_ref[1] + inv[look[2]] * vec_ref[2]
            )

    def exchange_start(x, table):
        def step(i, _):
            k = (i + 1) % pairs
            turned = rotate(k, gather(table, k))
            there = gather(table, pairs + k)
            for c in range(3):
                xsend[x, 0, k, c] = turned[c]
                xsend[x, 1, k, c] = there[c]

            if k != 0:
                send_back(x, k, behind_of[k]).start()
                send_ahead(x, k, ahead_of[k]).start()

            return 0

        loop(0, pairs, step, 0, pairs)
        later(1, pairs, lambda k: (send_back(x, k, b).wait_send(), send_ahead(x, k, b).wait_send()))
        xrecv[x, 0, 0] = xsend[x, 0, 0]
        xrecv[x, 1, 0] = xsend[x, 1, 0]

    def send_ahead(x, k, blk):
        return copy(xsend.at[x, 0, k], xrecv.at[x, 0, k], s_x.at[x, 0, k], r_x.at[x, 0, k], blk, r)

    def send_back(x, k, blk):
        return copy(xsend.at[x, 1, k], xrecv.at[x, 1, k], s_x.at[x, 1, k], r_x.at[x, 1, k], blk, r)

    def to_twin(src, dst, send, recv):
        both = copy(src, dst, send, recv, b, 1 - r)
        both.start()
        pending.append(both.wait_send)
        return both.wait_recv

    def wait_back(x, k):
        if k != 0:
            send_back(x, k, b).wait_recv()

    def wait_ahead(x, k):
        if k != 0:
            send_ahead(x, k, b).wait_recv()

    lane = lax.broadcasted_iota(jnp.int32, (1, LANES), 1)

    def one_pass(p, _):
        def near_sums(k, totals):
            m = [mis[0, k, c] for c in range(3)]
            cf = [conf[k, c] for c in range(3)]
            squares = cf[0] * m[0] * m[0] + cf[1] * m[1] * m[1] + cf[2] * m[2] * m[2]
            weight = live[k] / jnp.sqrt(squares + SOFTEN * SOFTEN)
            wout[k] = weight
            wc = [weight * cf[c] for c in range(3)]
            for c in range(3):
                wconf[0, k, c] = wc[c]
            back = rotate_back(k, [wc[c] * m[c] for c in range(3)])
            rot = [[rotm[k, 3 * i + j] for j in range(3)] for i in range(3)]
            terms = [-value for value in back]
            for f, s in DIAGONAL + OTHERS:
                terms.append(
                    rot[0][f] * wc[0] * rot[0][s]
                    + rot[1][f] * wc[1] * rot[1][s]
                    + rot[2][f] * wc[2] * rot[2][s]
                )
            put(k, 0, terms, k)
            return totals + dot_nt(lhs[k], hot[k])

        def far_sums(k, totals):
            m = [mis[1, k, c] for c in range(3)]
            cf = [recv1[k, c] for c in range(3)]
            squares = cf[0] * m[0] * m[0] + cf[1] * m[1] * m[1] + cf[2] * m[2] * m[2]
            weight = 1.0 / jnp.sqrt(squares + SOFTEN * SOFTEN)
            wc = [weight * cf[c] for c in range(3)]
            for c in range(3):
                wconf[1, k, c] = wc[c]
            put(pairs + k, 0, [wc[c] * m[c] for c in range(3)] + wc, pairs + k)
            return totals + dot_nt(lhs[pairs + k, 0 : 6 * rows_of], hot[pairs + k])

        near = loop(0, pairs, near_sums, jnp.zeros((9 * rows_of, lo_count), F32), US)
        for n in range(6, 9):
            bsend[p, n] = summed(near, n)
        finish_others = to_twin(bsend.at[p, 6:9], brecv.at[p, 6:9], s_b.at[p, 1], r_b.at[p, 1])
        far = loop(0, pairs, far_sums, jnp.zeros((6 * rows_of, lo_count), F32), US)
        for n in range(6):
            bsend[p, n] = summed(near, n) + summed(far, n)
        finish_first = to_twin(bsend.at[p, 0:6], brecv.at[p, 0:6], s_b.at[p, 0], r_b.at[p, 0])
        finish_others()
        finish_first()
        anchor = anc[...]
        for c in range(3):
            fr[c] = bsend[p, c] + brecv[p, c] - anchor * est[c]
        diagonal = [bsend[p, 3 + n] + brecv[p, 3 + n] + anchor for n in range(3)]
        others = [bsend[p, 6 + n] + brecv[p, 6 + n] for n in range(3)]
        blocks = [diagonal[0], others[0], others[1], diagonal[1], others[2], diagonal[2]]
        adjugate = [
            blocks[3] * blocks[5] - blocks[4] * blocks[4],
            blocks[2] * blocks[4] - blocks[1] * blocks[5],
            blocks[1] * blocks[4] - blocks[2] * blocks[3],
            blocks[0] * blocks[5] - blocks[2] * blocks[2],
            blocks[1] * blocks[2] - blocks[0] * blocks[4],
            blocks[0] * blocks[3] - blocks[1] * blocks[1],
        ]
        determinant = blocks[0] * adjugate[0] + blocks[1] * adjugate[1] + blocks[2] * adjugate[2]
        for n in range(6):
            inv[n] = adjugate[n] / determinant
        invert(fr, fz)

        x = 2 * p
        exchange_start(x, table_of(fz, 2))

        def product_near(k, totals):
            wait_back(x, k)
            change = [xrecv[x, 1, k, c] - xsend[x, 0, k, c] for c in range(3)]
            pushed = []
            square = totals[1]
            for c in range(3):
                chz[0, k, c] = change[c]
                pushed.append(wconf[0, k, c] * change[c])
                square = square + pushed[c] * change[c]
            put(k, 0, [-value for value in rotate_back(k, pushed)], k)
            return totals[0] + dot_nt(lhs[k, 0 : 3 * rows_of], hot[k]), square

        def product_far(k, totals):
            wait_ahead(x, k)
            change = [xsend[x, 1, k, c] - xrecv[x, 0, k, c] for c in range(3)]
            pushed = []
            for c in range(3):
                chz[1, k, c] = change[c]
                pushed.append(wconf[1, k, c] * change[c])
            put(pairs + k, 0, pushed, pairs + k)
            return totals + dot_nt(lhs[pairs + k, 0 : 3 * rows_of], hot[pairs + k])

        zero_row = jnp.zeros((tiles, LANES), F32)
        totals, z_square = loop(
            0, pairs, product_near, (jnp.zeros((3 * rows_of, lo_count), F32), zero_row), pairs
        )
        totals = loop(0, pairs, product_far, totals, pairs)
        for c in range(3):
            dsend[p, c] = summed(totals, c)
        to_twin(dsend.at[p], drecv.at[p], s_d.at[p], r_d.at[p])()
        for c in range(3):
            fq[c] = dsend[p, c] + drecv[p, c] + anchor * fz[c]
        invert(fq, fu)

        y = 2 * p + 1
        exchange_start(y, table_of(fu, 2))

        def change_u(k, square):
            wait_back(y, k)
            for c in range(3):
                change = xrecv[y, 1, k, c] - xsend[y, 0, k, c]
                chu[k, c] = change
                square = square + wconf[0, k, c] * change * change
            return square

        u_square = loop(0, pairs, change_u, zero_row, pairs)

        half = 1.0 / n_rep
        rz = fr[0] * fz[0] + fr[1] * fz[1] + fr[2] * fz[2]
        zz = anchor * (fz[0] * fz[0] + fz[1] * fz[1] + fz[2] * fz[2])
        uu = anchor * (fu[0] * fu[0] + fu[1] * fu[1] + fu[2] * fu[2])
        uq = fu[0] * fq[0] + fu[1] * fq[1] + fu[2] * fq[2]
        parts = (
            half * full_sum(rz),
            half * full_sum(zz) + full_sum(z_square),
            half * full_sum(uq),
            half * full_sum(uu) + full_sum(u_square),
        )
        row = jnp.zeros((1, LANES), F32)
        for n, part in enumerate(parts):
            row = jnp.where(lane == n, part, row)

        def reduce_over(row, send_ref, recv_ref, s_sem, r_sem, me, peers, meanwhile):
            count = len(peers)
            send_ref[p] = row

            def send(j, at, blk, rep):
                return copy(
                    send_ref.at[p], recv_ref.at[p, at], s_sem.at[p, j], r_sem.at[p, at], blk, rep
                )

            for j in range(1, count):
                send(j, me, *peers[j]).start()
            meanwhile()
            later(1, count, lambda j: send(j, me, b, r).wait_send())
            recv_ref[p, me] = row
            for j in range(1, count):
                send(j, lax.rem(me + j, count), b, r).wait_recv()
            total = recv_ref[p, 0]
            for n in range(1, count):
                total = total + recv_ref[p, n]
            return total

        def write_weights():
            drain()
            for k in range(pairs):
                for t in range(tiles):
                    weights_out[0, k : k + 1, t * LANES : (t + 1) * LANES] = wout[k, t : t + 1]

        row = reduce_over(row, g1send, g1recv, s_g1, r_g1, low, inner_of, drain)
        row = reduce_over(row, g2send, g2recv, s_g2, r_g2, mine2, outer_of, write_weights)

        def scalar(n):
            return jnp.sum(jnp.where(lane == n, row, 0.0), axis=1, keepdims=True)

        rz, zq, uq, uw = scalar(0), scalar(1), scalar(2), scalar(3)
        alpha = rz / zq
        norm_next = rz - 2.0 * alpha * zq + alpha * alpha * uq
        beta = norm_next / rz
        grown = 1.0 + beta
        along = grown * grown * zq - 2.0 * alpha * grown * uq + alpha * alpha * uw
        alpha_two = norm_next / along
        of_z = alpha + alpha_two * grown
        of_u = -alpha * alpha_two
        for c in range(3):
            est[c] = est[c] + of_z * fz[c] + of_u * fu[c]
        def new_misfit(k, _):
            wait_ahead(y, k)
            for c in range(3):
                mis[0, k, c] = mis[0, k, c] - of_z * chz[0, k, c] - of_u * chu[k, c]
                far_u = xsend[y, 1, k, c] - xrecv[y, 0, k, c]
                mis[1, k, c] = mis[1, k, c] - of_z * chz[1, k, c] - of_u * far_u
            return 0

        loop(0, pairs, new_misfit, 0, pairs)
        drain()
        return 0

    drain()
    lax.fori_loop(0, PASSES, one_pass, 0)

    for h in range(HI):
        at = slice(h * lo_count, (h + 1) * lo_count)
        for c in range(3):
            est_out[c : c + 1, at] = est[c, h : h + 1]


def on_device(
    n_blk,
    n_rep,
    measured,
    rot_vector,
    confidence,
    first_local,
    second_local,
    edge_counts,
    start_angles,
    anchor,
):
    pairs, slots = first_local.shape[1], first_local.shape[2]
    cams = start_angles.shape[1]
    tiles = slots // LANES
    lo = cams // HI
    wide = (n_blk // GROUP) * n_rep
    vmem = pltpu.VMEM
    sem = pltpu.SemaphoreType.DMA

    def edges(*lead):
        return vmem((*lead, tiles, LANES), F32)

    def cameras(*lead):
        return vmem((*lead, HI, lo), F32)

    scratch = [
        vmem((3 * pairs, lo, slots), BF16),
        vmem((3 * pairs, HI, slots), F32),
        vmem((3 * pairs, tiles, LANES), jnp.int32),
        edges(pairs, 9),
        edges(pairs, 3),
        edges(pairs, 3),
        edges(pairs),
        edges(pairs),
        edges(2, pairs, 3),
        edges(2, pairs, 3),
        edges(2, pairs, 3),
        edges(pairs, 3),
        edges(pairs, 4),
        edges(pairs, 4),
        edges(pairs, 3),
        edges(pairs, 3),
        cameras(3),
        cameras(pairs, 3),
        cameras(),
        cameras(6),
        cameras(3),
        cameras(3),
        cameras(3),
        cameras(3),
        cameras(PASSES, 9),
        cameras(PASSES, 9),
        cameras(PASSES, 3),
        cameras(PASSES, 3),
        edges(2 * PASSES, 2, pairs, 3),
        edges(2 * PASSES, 2, pairs, 3),
        vmem((PASSES, 1, LANES), F32),
        vmem((PASSES, GROUP, 1, LANES), F32),
        vmem((PASSES, 1, LANES), F32),
        vmem((PASSES, wide, 1, LANES), F32),
        vmem((2 * pairs, 18 * HI, slots), BF16),
        sem((3, pairs)),
        sem((3, pairs)),
        sem((PASSES, 2)),
        sem((PASSES, 2)),
        sem((PASSES,)),
        sem((PASSES,)),
        sem((2 * PASSES, 2, pairs)),
        sem((2 * PASSES, 2, pairs)),
        sem((PASSES, GROUP)),
        sem((PASSES, GROUP)),
        sem((PASSES, wide)),
        sem((PASSES, wide)),
        vmem(measured.shape, F32),
        vmem(rot_vector.shape, F32),
        vmem(confidence.shape, F32),
        vmem(first_local.shape, jnp.int32),
        vmem(second_local.shape, jnp.int32),
        vmem((1, pairs), jnp.int32),
        vmem(start_angles.shape, F32),
        vmem((1, cams), F32),
        sem((8,)),
    ]
    whole = pl.BlockSpec(memory_space=pltpu.VMEM)
    return pl.pallas_call(
        functools.partial(kernel, n_blk, n_rep),
        out_shape=(
            pltpu.VMEM((3, cams), F32),
            pltpu.VMEM((1, pairs, slots), F32),
        ),
        in_specs=[pl.BlockSpec(memory_space=pl.ANY)] * 8,
        out_specs=(whole, whole),
        scratch_shapes=scratch,
        compiler_params=pltpu.CompilerParams(
            collective_id=0, has_side_effects=True, vmem_limit_bytes=60 * 1024 * 1024
        ),
    )(
        measured,
        rot_vector,
        confidence,
        first_local,
        second_local,
        edge_counts.reshape(1, -1),
        start_angles,
        anchor.reshape(1, -1),
    )


def solution(mesh):
    return jax.shard_map(
        functools.partial(on_device, mesh.shape["blk"], mesh.shape["rep"]),
        mesh=mesh,
        in_specs=(
            P(None, "blk", None, "rep"),
            P(None, "blk", None, "rep"),
            P(None, "blk", None, "rep"),
            P("blk", None, "rep"),
            P("blk", None, "rep"),
            P("blk", None, "rep"),
            P(None, "blk"),
            P("blk"),
        ),
        out_specs=(P(None, "blk"), P("blk", None, "rep")),
        check_vma=False,
    )
```

```python
import functools

import jax
import jax.numpy as jnp
from jax import lax
from jax.experimental import pallas as pl
from jax.experimental.pallas import tpu as pltpu
from jax.sharding import PartitionSpec as P

PASSES = 2
SOFTEN = 0.05
MESH = pl.DeviceIdType.MESH
LANES = 128
HI = 16
DIAGONAL = ((0, 0), (1, 1), (2, 2))
OTHERS = ((0, 1), (0, 2), (1, 2))
F32 = jnp.float32
BF16 = jnp.bfloat16


UG = 8
US = 4
UB = 4
UJ = 8


def loop(first, last, body, init, unroll):
    if unroll < last - first:
        return lax.fori_loop(first, last, body, init, unroll=unroll)
    for i in range(first, last):
        init = body(i, init)
    return init


def dot_nn(a, b):
    return lax.dot_general(a, b, (((1,), (0,)), ((), ())), preferred_element_type=F32)


def dot_nt(a, b):
    return lax.dot_general(a, b, (((1,), (1,)), ((), ())), preferred_element_type=F32)


def pieces_of(value, count):
    found = []
    for _ in range(count - 1):
        found.append(value.astype(BF16).astype(F32))
        value = value - found[-1]
    return found + [value]


def kernel(
    n_blk,
    n_rep,
    measured_in,
    rot_in,
    conf_in,
    first_in,
    second_in,
    counts_in,
    start_in,
    anchor_in,
    est_out,
    weights_out,
    hot,
    himask,
    idx,
    rotm,
    meas,
    conf,
    live,
    wout,
    mis,
    wconf,
    chz,
    chu,
    send1,
    recv1,
    send2,
    recv2,
    est,
    halo,
    anc,
    inv,
    fz,
    fu,
    fr,
    fq,
    bsend,
    brecv,
    dsend,
    drecv,
    xsend,
    xrecv,
    gsend,
    grecv,
    lhs,
    s_init,
    r_init,
    s_b,
    r_b,
    s_d,
    r_d,
    s_x,
    r_x,
    s_g,
    r_g,
    measured_ref,
    rot_ref,
    conf_ref,
    first_ref,
    second_ref,
    counts_ref,
    start_ref,
    anchor_ref,
    s_in,
):
    pairs = idx.shape[0] // 3
    tiles = idx.shape[1]
    rows_of = 2 * HI
    lo_count = est.shape[2]
    b = lax.axis_index("blk")
    r = lax.axis_index("rep")

    def ahead(k):
        return lax.rem(b + k, n_blk)

    def behind(k):
        return lax.rem(b + n_blk - k, n_blk)

    def copy(src, dst, send, recv, blk, rep):
        return pltpu.make_async_remote_copy(
            src_ref=src,
            dst_ref=dst,
            send_sem=send,
            recv_sem=recv,
            device_id={"blk": blk, "rep": rep},
            device_id_type=MESH,
        )

    pending = []

    def drain():
        while pending:
            pending.pop(0)()

    def later(first, last, wait):
        def loop():
            def step(k, _):
                wait(k)
                return 0

            lax.fori_loop(first, last, step, 0)

        pending.append(loop)

    loads = [
        pltpu.make_async_copy(src, dst, s_in.at[n])
        for n, (src, dst) in enumerate(
            (
                (start_in, start_ref),
                (second_in, second_ref),
                (conf_in, conf_ref),
                (counts_in, counts_ref),
                (first_in, first_ref),
                (rot_in, rot_ref),
                (measured_in, measured_ref),
                (anchor_in, anchor_ref),
            )
        )
    ]
    for load in loads:
        load.start()

    barrier = pltpu.get_barrier_semaphore()

    ahead_of = [ahead(k) for k in range(pairs)]
    behind_of = [behind(k) for k in range(pairs)]
    count = n_blk * n_rep
    me = b * n_rep + r

    def greet(j, _):
        pl.semaphore_signal(
            barrier, inc=1, device_id=lax.rem(me + j, count), device_id_type=pl.DeviceIdType.LOGICAL
        )
        return 0

    lax.fori_loop(1, count, greet, 0, unroll=UJ)

    for load in loads:
        load.wait()
    slot = lax.broadcasted_iota(jnp.int32, (tiles, LANES), 0) * LANES
    slot = slot + lax.broadcasted_iota(jnp.int32, (tiles, LANES), 1)
    for k in range(pairs):
        live[k] = jnp.where(slot < counts_ref[0:1, k : k + 1], 1.0, 0.0).astype(F32)
        for t in range(tiles):
            at = slice(t * LANES, (t + 1) * LANES)
            idx[k, t : t + 1] = first_ref[0, k : k + 1, at]
            idx[2 * pairs + k, t : t + 1] = second_ref[0, k : k + 1, at]
            for c in range(3):
                conf[k, c, t : t + 1] = conf_ref[c, 0, k : k + 1, at]
                meas[k, c, t : t + 1] = measured_ref[c, 0, k : k + 1, at]
                rotm[k, c, t : t + 1] = rot_ref[c, 0, k : k + 1, at]
    for h in range(HI):
        at = slice(h * lo_count, (h + 1) * lo_count)
        anc[h : h + 1] = anchor_ref[0:1, at]
        for c in range(3):
            est[c, h : h + 1] = start_ref[c : c + 1, at]

    def stage1(k, _):
        for c in range(3):
            conf[k, c] = conf[k, c] * live[k]
            send1[k, c] = conf[k, c]
        send1[k, 3] = idx[2 * pairs + k].astype(F32)
        return 0

    lax.fori_loop(0, pairs, stage1, 0)
    halo[0] = est[...]

    def send_init(k, blk):
        return copy(send1.at[k], recv1.at[k], s_init.at[0, k], r_init.at[0, k], blk, r)

    def send_mis(k, blk):
        return copy(send2.at[k], recv2.at[k], s_init.at[1, k], r_init.at[1, k], blk, r)

    def send_halo(k, blk):
        return copy(halo.at[0], halo.at[k], s_init.at[2, k], r_init.at[2, k], blk, r)

    pl.semaphore_wait(barrier, count - 1)
    for k in range(1, pairs):
        send_halo(k, behind_of[k]).start()
        send_init(k, ahead_of[k]).start()

    def rotations(k, _):
        v = [rotm[k, c] for c in range(3)]
        squared = v[0] * v[0] + v[1] * v[1] + v[2] * v[2]
        factor = 2.0 / (1.0 + squared)
        zero = jnp.zeros_like(squared)
        skew = ((zero, -v[2], v[1]), (v[2], zero, -v[0]), (-v[1], v[0], zero))
        for i in range(3):
            for j in range(3):
                term = skew[i][j] + v[i] * v[j]
                if i == j:
                    rotm[k, 3 * i + j] = 1.0 + factor * (term - squared)
                else:
                    rotm[k, 3 * i + j] = factor * term
        return 0

    lax.fori_loop(0, pairs, rotations, 0)

    def build(g):
        for t in range(tiles):
            where = idx[g, t : t + 1]
            low_part = lax.rem(where, lo_count)
            high_part = where // lo_count
            at = slice(t * LANES, (t + 1) * LANES)
            himask[g, :, at] = jnp.where(
                lax.broadcasted_iota(jnp.int32, (HI, LANES), 0) == high_part, 1.0, 0.0
            ).astype(F32)
            hot[g, :, at] = jnp.where(
                lax.broadcasted_iota(jnp.int32, (lo_count, LANES), 0) == low_part, 1.0, 0.0
            ).astype(BF16)

    def build_near(k, _):
        build(k)
        return 0

    def build_second(k, _):
        build(2 * pairs + k)
        return 0

    def table_of(field, count):
        rows = []
        for c in range(3):
            rows.extend(pieces_of(field[c], count))
        return jnp.concatenate(rows, axis=0).astype(BF16)

    def gather(table, g):
        full = dot_nn(table, hot[g])
        mask = himask[g]
        count = table.shape[0] // (3 * HI)
        found = []
        for c in range(3):
            part = full[HI * count * c : HI * count * c + HI]
            for n in range(1, count):
                part = part + full[HI * (count * c + n) : HI * (count * c + n + 1)]
            part = part * mask
            row = jnp.sum(part, axis=0, keepdims=True)
            found.append(
                jnp.concatenate([row[:, t * LANES : (t + 1) * LANES] for t in range(tiles)], axis=0)
            )
        return found

    def rotate(k, vec):
        return [
            rotm[k, 3 * i] * vec[0] + rotm[k, 3 * i + 1] * vec[1] + rotm[k, 3 * i + 2] * vec[2]
            for i in range(3)
        ]

    def rotate_back(k, vec):
        return [
            rotm[k, i] * vec[0] + rotm[k, 3 + i] * vec[1] + rotm[k, 6 + i] * vec[2]
            for i in range(3)
        ]

    loop(0, pairs, build_near, 0, UB)
    table = table_of(est, 3)

    def near_start(k, _):
        turned = rotate(k, gather(table, k))
        for c in range(3):
            send2[k, c] = meas[k, c] + turned[c]
        if k != 0:
            send_mis(k, ahead_of[k]).start()
        return 0

    loop(0, pairs, near_start, 0, pairs)
    loop(0, pairs, build_second, 0, UB)
    later(
        1,
        pairs,
        lambda k: [send(k, b).wait_send() for send in (send_init, send_mis, send_halo)],
    )
    recv1[0] = send1[0]
    recv2[0] = send2[0]

    for k in range(1, pairs):
        send_init(k, b).wait_recv()

    def build_far(k, _):
        idx[pairs + k] = recv1[k, 3].astype(jnp.int32)
        build(pairs + k)
        return 0

    loop(0, pairs, build_far, 0, UB)

    def far_misfit(k, _):
        there = gather(table, pairs + k)
        for c in range(3):
            mis[1, k, c] = recv2[k, c] - there[c]
        return 0

    for k in range(1, pairs):
        send_mis(k, b).wait_recv()
    loop(0, pairs, far_misfit, 0, UG)
    for k in range(1, pairs):
        send_halo(k, b).wait_recv()

    def own_misfit(k, _):
        there = gather(table_of(halo.at[k], 3), 2 * pairs + k)
        for c in range(3):
            mis[0, k, c] = send2[k, c] - there[c]
        return 0

    loop(0, pairs, own_misfit, 0, UG)

    def put(slot, at_row, terms, g):
        for n, term in enumerate(terms):
            head, tail = pieces_of(term, 2)
            for t in range(tiles):
                at = slice(t * LANES, (t + 1) * LANES)
                mask = himask[g, :, at]
                both = jnp.concatenate([head[t : t + 1] * mask, tail[t : t + 1] * mask], axis=0)
                lhs[slot, at_row + rows_of * n : at_row + rows_of * (n + 1), at] = both.astype(BF16)

    def summed(totals, channel):
        at = rows_of * channel
        return totals[at : at + HI] + totals[at + HI : at + rows_of]

    def full_sum(value):
        return jnp.sum(jnp.sum(value, axis=0, keepdims=True), axis=1, keepdims=True)

    def invert(vec_ref, out_ref):
        for i in range(3):
            look = ((0, 1, 2), (1, 3, 4), (2, 4, 5))[i]
            out_ref[i] = (
                inv[look[0]] * vec_ref[0] + inv[look[1]] * vec_ref[1] + inv[look[2]] * vec_ref[2]
            )

    def exchange_start(x, table):
        def step(i, _):
            k = (i + 1) % pairs
            turned = rotate(k, gather(table, k))
            there = gather(table, pairs + k)
            for c in range(3):
                xsend[x, 0, k, c] = turned[c]
                xsend[x, 1, k, c] = there[c]

            if k != 0:
                send_back(x, k, behind_of[k]).start()
                send_ahead(x, k, ahead_of[k]).start()

            return 0

        loop(0, pairs, step, 0, pairs)
        later(1, pairs, lambda k: (send_back(x, k, b).wait_send(), send_ahead(x, k, b).wait_send()))
        xrecv[x, 0, 0] = xsend[x, 0, 0]
        xrecv[x, 1, 0] = xsend[x, 1, 0]

    def send_ahead(x, k, blk):
        return copy(xsend.at[x, 0, k], xrecv.at[x, 0, k], s_x.at[x, 0, k], r_x.at[x, 0, k], blk, r)

    def send_back(x, k, blk):
        return copy(xsend.at[x, 1, k], xrecv.at[x, 1, k], s_x.at[x, 1, k], r_x.at[x, 1, k], blk, r)

    def to_twin(src, dst, send, recv):
        both = copy(src, dst, send, recv, b, 1 - r)
        both.start()
        pending.append(both.wait_send)
        return both.wait_recv

    def wait_back(x, k):
        if k != 0:
            send_back(x, k, b).wait_recv()

    def wait_ahead(x, k):
        if k != 0:
            send_ahead(x, k, b).wait_recv()

    lane = lax.broadcasted_iota(jnp.int32, (1, LANES), 1)

    def one_pass(p, _):
        def near_sums(k, totals):
            m = [mis[0, k, c] for c in range(3)]
            cf = [conf[k, c] for c in range(3)]
            squares = cf[0] * m[0] * m[0] + cf[1] * m[1] * m[1] + cf[2] * m[2] * m[2]
            weight = live[k] / jnp.sqrt(squares + SOFTEN * SOFTEN)
            wout[k] = weight
            wc = [weight * cf[c] for c in range(3)]
            for c in range(3):
                wconf[0, k, c] = wc[c]
            back = rotate_back(k, [wc[c] * m[c] for c in range(3)])
            rot = [[rotm[k, 3 * i + j] for j in range(3)] for i in range(3)]
            terms = [-value for value in back]
            for f, s in DIAGONAL + OTHERS:
                terms.append(
                    rot[0][f] * wc[0] * rot[0][s]
                    + rot[1][f] * wc[1] * rot[1][s]
                    + rot[2][f] * wc[2] * rot[2][s]
                )
            put(k, 0, terms, k)
            return totals + dot_nt(lhs[k], hot[k])

        def far_sums(k, totals):
            m = [mis[1, k, c] for c in range(3)]
            cf = [recv1[k, c] for c in range(3)]
            squares = cf[0] * m[0] * m[0] + cf[1] * m[1] * m[1] + cf[2] * m[2] * m[2]
            weight = 1.0 / jnp.sqrt(squares + SOFTEN * SOFTEN)
            wc = [weight * cf[c] for c in range(3)]
            for c in range(3):
                wconf[1, k, c] = wc[c]
            put(pairs + k, 0, [wc[c] * m[c] for c in range(3)] + wc, pairs + k)
            return totals + dot_nt(lhs[pairs + k, 0 : 6 * rows_of], hot[pairs + k])

        near = loop(0, pairs, near_sums, jnp.zeros((9 * rows_of, lo_count), F32), US)
        for n in range(6, 9):
            bsend[p, n] = summed(near, n)
        finish_others = to_twin(bsend.at[p, 6:9], brecv.at[p, 6:9], s_b.at[p, 1], r_b.at[p, 1])
        far = loop(0, pairs, far_sums, jnp.zeros((6 * rows_of, lo_count), F32), US)
        for n in range(6):
            bsend[p, n] = summed(near, n) + summed(far, n)
        finish_first = to_twin(bsend.at[p, 0:6], brecv.at[p, 0:6], s_b.at[p, 0], r_b.at[p, 0])
        finish_others()
        finish_first()
        anchor = anc[...]
        for c in range(3):
            fr[c] = bsend[p, c] + brecv[p, c] - anchor * est[c]
        diagonal = [bsend[p, 3 + n] + brecv[p, 3 + n] + anchor for n in range(3)]
        others = [bsend[p, 6 + n] + brecv[p, 6 + n] for n in range(3)]
        blocks = [diagonal[0], others[0], others[1], diagonal[1], others[2], diagonal[2]]
        adjugate = [
            blocks[3] * blocks[5] - blocks[4] * blocks[4],
            blocks[2] * blocks[4] - blocks[1] * blocks[5],
            blocks[1] * blocks[4] - blocks[2] * blocks[3],
            blocks[0] * blocks[5] - blocks[2] * blocks[2],
            blocks[1] * blocks[2] - blocks[0] * blocks[4],
            blocks[0] * blocks[3] - blocks[1] * blocks[1],
        ]
        determinant = blocks[0] * adjugate[0] + blocks[1] * adjugate[1] + blocks[2] * adjugate[2]
        for n in range(6):
            inv[n] = adjugate[n] / determinant
        invert(fr, fz)

        x = 2 * p
        exchange_start(x, table_of(fz, 2))

        def product_near(k, totals):
            wait_back(x, k)
            change = [xrecv[x, 1, k, c] - xsend[x, 0, k, c] for c in range(3)]
            pushed = []
            square = totals[1]
            for c in range(3):
                chz[0, k, c] = change[c]
                pushed.append(wconf[0, k, c] * change[c])
                square = square + pushed[c] * change[c]
            put(k, 0, [-value for value in rotate_back(k, pushed)], k)
            return totals[0] + dot_nt(lhs[k, 0 : 3 * rows_of], hot[k]), square

        def product_far(k, totals):
            wait_ahead(x, k)
            change = [xsend[x, 1, k, c] - xrecv[x, 0, k, c] for c in range(3)]
            pushed = []
            for c in range(3):
                chz[1, k, c] = change[c]
                pushed.append(wconf[1, k, c] * change[c])
            put(pairs + k, 0, pushed, pairs + k)
            return totals + dot_nt(lhs[pairs + k, 0 : 3 * rows_of], hot[pairs + k])

        zero_row = jnp.zeros((tiles, LANES), F32)
        totals, z_square = loop(
            0, pairs, product_near, (jnp.zeros((3 * rows_of, lo_count), F32), zero_row), pairs
        )
        totals = loop(0, pairs, product_far, totals, pairs)
        for c in range(3):
            dsend[p, c] = summed(totals, c)
        to_twin(dsend.at[p], drecv.at[p], s_d.at[p], r_d.at[p])()
        for c in range(3):
            fq[c] = dsend[p, c] + drecv[p, c] + anchor * fz[c]
        invert(fq, fu)

        y = 2 * p + 1
        exchange_start(y, table_of(fu, 2))

        def change_u(k, square):
            wait_back(y, k)
            for c in range(3):
                change = xrecv[y, 1, k, c] - xsend[y, 0, k, c]
                chu[k, c] = change
                square = square + wconf[0, k, c] * change * change
            return square

        u_square = loop(0, pairs, change_u, zero_row, pairs)

        half = 1.0 / n_rep
        rz = fr[0] * fz[0] + fr[1] * fz[1] + fr[2] * fz[2]
        zz = anchor * (fz[0] * fz[0] + fz[1] * fz[1] + fz[2] * fz[2])
        uu = anchor * (fu[0] * fu[0] + fu[1] * fu[1] + fu[2] * fu[2])
        uq = fu[0] * fq[0] + fu[1] * fq[1] + fu[2] * fq[2]
        parts = (
            half * full_sum(rz),
            half * full_sum(zz) + full_sum(z_square),
            half * full_sum(uq),
            half * full_sum(uu) + full_sum(u_square),
        )
        row = jnp.zeros((1, LANES), F32)
        for n, part in enumerate(parts):
            row = jnp.where(lane == n, part, row)

        def reduce_all(row, meanwhile):
            gsend[p] = row

            def start(j, _):
                pltpu.make_async_remote_copy(
                    src_ref=gsend.at[p],
                    dst_ref=grecv.at[p, me],
                    send_sem=s_g.at[p],
                    recv_sem=r_g.at[p],
                    device_id=lax.rem(me + j, count),
                    device_id_type=pl.DeviceIdType.LOGICAL,
                ).start()
                return 0

            lax.fori_loop(1, count, start, 0, unroll=UJ)
            meanwhile()
            grecv[p, me] = row
            rest = pltpu.make_async_copy(grecv.at[p, 1:count], grecv.at[p, 1:count], r_g.at[p])
            rest.wait()
            sent = pltpu.make_async_copy(grecv.at[p, 1:count], grecv.at[p, 1:count], s_g.at[p])
            pending.append(sent.wait)
            total = [grecv[p, n] for n in range(8)]
            for n in range(8, count):
                total[n % 8] = total[n % 8] + grecv[p, n]
            total = [total[n] + total[n + 4] for n in range(4)]
            return (total[0] + total[1]) + (total[2] + total[3])

        def write_weights():
            drain()
            for k in range(pairs):
                for t in range(tiles):
                    weights_out[0, k : k + 1, t * LANES : (t + 1) * LANES] = wout[k, t : t + 1]

        row = reduce_all(row, write_weights)

        def scalar(n):
            return jnp.sum(jnp.where(lane == n, row, 0.0), axis=1, keepdims=True)

        rz, zq, uq, uw = scalar(0), scalar(1), scalar(2), scalar(3)
        alpha = rz / zq
        norm_next = rz - 2.0 * alpha * zq + alpha * alpha * uq
        beta = norm_next / rz
        grown = 1.0 + beta
        along = grown * grown * zq - 2.0 * alpha * grown * uq + alpha * alpha * uw
        alpha_two = norm_next / along
        of_z = alpha + alpha_two * grown
        of_u = -alpha * alpha_two
        for c in range(3):
            est[c] = est[c] + of_z * fz[c] + of_u * fu[c]
        def new_misfit(k, _):
            wait_ahead(y, k)
            for c in range(3):
                mis[0, k, c] = mis[0, k, c] - of_z * chz[0, k, c] - of_u * chu[k, c]
                far_u = xsend[y, 1, k, c] - xrecv[y, 0, k, c]
                mis[1, k, c] = mis[1, k, c] - of_z * chz[1, k, c] - of_u * far_u
            return 0

        loop(0, pairs, new_misfit, 0, pairs)
        drain()
        return 0

    drain()
    lax.fori_loop(0, PASSES, one_pass, 0)

    for h in range(HI):
        at = slice(h * lo_count, (h + 1) * lo_count)
        for c in range(3):
            est_out[c : c + 1, at] = est[c, h : h + 1]


def on_device(
    n_blk,
    n_rep,
    measured,
    rot_vector,
    confidence,
    first_local,
    second_local,
    edge_counts,
    start_angles,
    anchor,
):
    pairs, slots = first_local.shape[1], first_local.shape[2]
    cams = start_angles.shape[1]
    tiles = slots // LANES
    lo = cams // HI
    vmem = pltpu.VMEM
    sem = pltpu.SemaphoreType.DMA

    def edges(*lead):
        return vmem((*lead, tiles, LANES), F32)

    def cameras(*lead):
        return vmem((*lead, HI, lo), F32)

    scratch = [
        vmem((3 * pairs, lo, slots), BF16),
        vmem((3 * pairs, HI, slots), F32),
        vmem((3 * pairs, tiles, LANES), jnp.int32),
        edges(pairs, 9),
        edges(pairs, 3),
        edges(pairs, 3),
        edges(pairs),
        edges(pairs),
        edges(2, pairs, 3),
        edges(2, pairs, 3),
        edges(2, pairs, 3),
        edges(pairs, 3),
        edges(pairs, 4),
        edges(pairs, 4),
        edges(pairs, 3),
        edges(pairs, 3),
        cameras(3),
        cameras(pairs, 3),
        cameras(),
        cameras(6),
        cameras(3),
        cameras(3),
        cameras(3),
        cameras(3),
        cameras(PASSES, 9),
        cameras(PASSES, 9),
        cameras(PASSES, 3),
        cameras(PASSES, 3),
        edges(2 * PASSES, 2, pairs, 3),
        edges(2 * PASSES, 2, pairs, 3),
        vmem((PASSES, 1, LANES), F32),
        vmem((PASSES, n_blk * n_rep, 1, LANES), F32),
        vmem((2 * pairs, 18 * HI, slots), BF16),
        sem((3, pairs)),
        sem((3, pairs)),
        sem((PASSES, 2)),
        sem((PASSES, 2)),
        sem((PASSES,)),
        sem((PASSES,)),
        sem((2 * PASSES, 2, pairs)),
        sem((2 * PASSES, 2, pairs)),
        sem((PASSES,)),
        sem((PASSES,)),
        vmem(measured.shape, F32),
        vmem(rot_vector.shape, F32),
        vmem(confidence.shape, F32),
        vmem(first_local.shape, jnp.int32),
        vmem(second_local.shape, jnp.int32),
        vmem((1, pairs), jnp.int32),
        vmem(start_angles.shape, F32),
        vmem((1, cams), F32),
        sem((8,)),
    ]
    whole = pl.BlockSpec(memory_space=pltpu.VMEM)
    return pl.pallas_call(
        functools.partial(kernel, n_blk, n_rep),
        out_shape=(
            pltpu.VMEM((3, cams), F32),
            pltpu.VMEM((1, pairs, slots), F32),
        ),
        in_specs=[pl.BlockSpec(memory_space=pl.ANY)] * 8,
        out_specs=(whole, whole),
        scratch_shapes=scratch,
        compiler_params=pltpu.CompilerParams(
            collective_id=0, has_side_effects=True, vmem_limit_bytes=60 * 1024 * 1024
        ),
    )(
        measured,
        rot_vector,
        confidence,
        first_local,
        second_local,
        edge_counts.reshape(1, -1),
        start_angles,
        anchor.reshape(1, -1),
    )


def solution(mesh):
    return jax.shard_map(
        functools.partial(on_device, mesh.shape["blk"], mesh.shape["rep"]),
        mesh=mesh,
        in_specs=(
            P(None, "blk", None, "rep"),
            P(None, "blk", None, "rep"),
            P(None, "blk", None, "rep"),
            P("blk", None, "rep"),
            P("blk", None, "rep"),
            P("blk", None, "rep"),
            P(None, "blk"),
            P("blk"),
        ),
        out_specs=(P(None, "blk"), P("blk", None, "rep")),
        check_vma=False,
    )
```

```python
import functools

import jax
import jax.numpy as jnp
from jax import lax
from jax.experimental import pallas as pl
from jax.experimental.pallas import tpu as pltpu
from jax.sharding import PartitionSpec as P

PASSES = 2
SOFTEN = 0.05
MESH = pl.DeviceIdType.MESH
LANES = 128
HI = 16
DIAGONAL = ((0, 0), (1, 1), (2, 2))
OTHERS = ((0, 1), (0, 2), (1, 2))
F32 = jnp.float32
BF16 = jnp.bfloat16


UG = 8
US = 4
UB = 4
UJ = 16


def loop(first, last, body, init, unroll):
    if unroll < last - first:
        return lax.fori_loop(first, last, body, init, unroll=unroll)
    for i in range(first, last):
        init = body(i, init)
    return init


def dot_nn(a, b):
    return lax.dot_general(a, b, (((1,), (0,)), ((), ())), preferred_element_type=F32)


def dot_nt(a, b):
    return lax.dot_general(a, b, (((1,), (1,)), ((), ())), preferred_element_type=F32)


def pieces_of(value, count):
    found = []
    for _ in range(count - 1):
        found.append(value.astype(BF16).astype(F32))
        value = value - found[-1]
    return found + [value]


def kernel(
    n_blk,
    n_rep,
    measured_in,
    rot_in,
    conf_in,
    first_in,
    second_in,
    counts_in,
    start_in,
    anchor_in,
    est_out,
    weights_out,
    hot,
    himask,
    idx,
    rotm,
    meas,
    conf,
    live,
    wout,
    mis,
    wconf,
    chz,
    chu,
    send1,
    recv1,
    send2,
    recv2,
    est,
    halo,
    anc,
    inv,
    fz,
    fu,
    fr,
    fq,
    bsend,
    brecv,
    dsend,
    drecv,
    xsend,
    xrecv,
    gsend,
    grecv,
    lhs,
    s_init,
    r_init,
    s_b,
    r_b,
    s_d,
    r_d,
    s_x,
    r_x,
    s_g,
    r_g,
    measured_ref,
    rot_ref,
    conf_ref,
    first_ref,
    second_ref,
    counts_ref,
    start_ref,
    anchor_ref,
    s_in,
):
    pairs = idx.shape[0] // 3
    tiles = idx.shape[1]
    rows_of = 2 * HI
    lo_count = est.shape[2]
    b = lax.axis_index("blk")
    r = lax.axis_index("rep")

    def ahead(k):
        return lax.rem(b + k, n_blk)

    def behind(k):
        return lax.rem(b + n_blk - k, n_blk)

    def copy(src, dst, send, recv, blk, rep):
        return pltpu.make_async_remote_copy(
            src_ref=src,
            dst_ref=dst,
            send_sem=send,
            recv_sem=recv,
            device_id={"blk": blk, "rep": rep},
            device_id_type=MESH,
        )

    pending = []

    def drain():
        while pending:
            pending.pop(0)()

    def later(first, last, wait):
        def loop():
            def step(k, _):
                wait(k)
                return 0

            lax.fori_loop(first, last, step, 0)

        pending.append(loop)

    loads = [
        pltpu.make_async_copy(src, dst, s_in.at[n])
        for n, (src, dst) in enumerate(
            (
                (start_in, start_ref),
                (second_in, second_ref),
                (conf_in, conf_ref),
                (counts_in, counts_ref),
                (first_in, first_ref),
                (rot_in, rot_ref),
                (measured_in, measured_ref),
                (anchor_in, anchor_ref),
            )
        )
    ]
    for load in loads:
        load.start()

    barrier = pltpu.get_barrier_semaphore()

    ahead_of = [ahead(k) for k in range(pairs)]
    behind_of = [behind(k) for k in range(pairs)]
    count = n_blk * n_rep
    me = b * n_rep + r

    def greet(j, _):
        pl.semaphore_signal(
            barrier, inc=1, device_id=lax.rem(me + j, count), device_id_type=pl.DeviceIdType.LOGICAL
        )
        return 0

    lax.fori_loop(1, count, greet, 0, unroll=UJ)

    for load in loads[:4]:
        load.wait()
    slot = lax.broadcasted_iota(jnp.int32, (tiles, LANES), 0) * LANES
    slot = slot + lax.broadcasted_iota(jnp.int32, (tiles, LANES), 1)
    for h in range(HI):
        at = slice(h * lo_count, (h + 1) * lo_count)
        for c in range(3):
            est[c, h : h + 1] = start_ref[c : c + 1, at]
    for k in range(pairs):
        live[k] = jnp.where(slot < counts_ref[0:1, k : k + 1], 1.0, 0.0).astype(F32)
        for t in range(tiles):
            at = slice(t * LANES, (t + 1) * LANES)
            idx[2 * pairs + k, t : t + 1] = second_ref[0, k : k + 1, at]
            for c in range(3):
                conf[k, c, t : t + 1] = conf_ref[c, 0, k : k + 1, at]

    def stage1(k, _):
        for c in range(3):
            conf[k, c] = conf[k, c] * live[k]
            send1[k, c] = conf[k, c]
        send1[k, 3] = idx[2 * pairs + k].astype(F32)
        return 0

    lax.fori_loop(0, pairs, stage1, 0)
    halo[0] = est[...]

    def send_init(k, blk):
        return copy(send1.at[k], recv1.at[k], s_init.at[0, k], r_init.at[0, k], blk, r)

    def send_mis(k, blk):
        return copy(send2.at[k], recv2.at[k], s_init.at[1, k], r_init.at[1, k], blk, r)

    def send_halo(k, blk):
        return copy(halo.at[0], halo.at[k], s_init.at[2, k], r_init.at[2, k], blk, r)

    pl.semaphore_wait(barrier, count - 1)
    for k in range(1, pairs):
        send_halo(k, behind_of[k]).start()
        send_init(k, ahead_of[k]).start()

    for load in loads[4:]:
        load.wait()
    for k in range(pairs):
        for t in range(tiles):
            at = slice(t * LANES, (t + 1) * LANES)
            idx[k, t : t + 1] = first_ref[0, k : k + 1, at]
            for c in range(3):
                meas[k, c, t : t + 1] = measured_ref[c, 0, k : k + 1, at]
                rotm[k, c, t : t + 1] = rot_ref[c, 0, k : k + 1, at]
    for h in range(HI):
        anc[h : h + 1] = anchor_ref[0:1, h * lo_count : (h + 1) * lo_count]

    def rotations(k, _):
        v = [rotm[k, c] for c in range(3)]
        squared = v[0] * v[0] + v[1] * v[1] + v[2] * v[2]
        factor = 2.0 / (1.0 + squared)
        zero = jnp.zeros_like(squared)
        skew = ((zero, -v[2], v[1]), (v[2], zero, -v[0]), (-v[1], v[0], zero))
        for i in range(3):
            for j in range(3):
                term = skew[i][j] + v[i] * v[j]
                if i == j:
                    rotm[k, 3 * i + j] = 1.0 + factor * (term - squared)
                else:
                    rotm[k, 3 * i + j] = factor * term
        return 0

    lax.fori_loop(0, pairs, rotations, 0)

    def build(g):
        for t in range(tiles):
            where = idx[g, t : t + 1]
            low_part = lax.rem(where, lo_count)
            high_part = where // lo_count
            at = slice(t * LANES, (t + 1) * LANES)
            himask[g, :, at] = jnp.where(
                lax.broadcasted_iota(jnp.int32, (HI, LANES), 0) == high_part, 1.0, 0.0
            ).astype(F32)
            hot[g, :, at] = jnp.where(
                lax.broadcasted_iota(jnp.int32, (lo_count, LANES), 0) == low_part, 1.0, 0.0
            ).astype(BF16)

    def build_near(k, _):
        build(k)
        return 0

    def build_second(k, _):
        build(2 * pairs + k)
        return 0

    def table_of(field, count):
        rows = []
        for c in range(3):
            rows.extend(pieces_of(field[c], count))
        return jnp.concatenate(rows, axis=0).astype(BF16)

    def gather(table, g):
        full = dot_nn(table, hot[g])
        mask = himask[g]
        count = table.shape[0] // (3 * HI)
        found = []
        for c in range(3):
            part = full[HI * count * c : HI * count * c + HI]
            for n in range(1, count):
                part = part + full[HI * (count * c + n) : HI * (count * c + n + 1)]
            part = part * mask
            row = jnp.sum(part, axis=0, keepdims=True)
            found.append(
                jnp.concatenate([row[:, t * LANES : (t + 1) * LANES] for t in range(tiles)], axis=0)
            )
        return found

    def rotate(k, vec):
        return [
            rotm[k, 3 * i] * vec[0] + rotm[k, 3 * i + 1] * vec[1] + rotm[k, 3 * i + 2] * vec[2]
            for i in range(3)
        ]

    def rotate_back(k, vec):
        return [
            rotm[k, i] * vec[0] + rotm[k, 3 + i] * vec[1] + rotm[k, 6 + i] * vec[2]
            for i in range(3)
        ]

    loop(0, pairs, build_near, 0, UB)
    table = table_of(est, 3)

    def near_start(k, _):
        turned = rotate(k, gather(table, k))
        for c in range(3):
            send2[k, c] = meas[k, c] + turned[c]
        if k != 0:
            send_mis(k, ahead_of[k]).start()
        return 0

    loop(0, pairs, near_start, 0, pairs)
    loop(0, pairs, build_second, 0, UB)
    later(
        1,
        pairs,
        lambda k: [send(k, b).wait_send() for send in (send_init, send_mis, send_halo)],
    )
    recv1[0] = send1[0]
    recv2[0] = send2[0]

    for k in range(1, pairs):
        send_init(k, b).wait_recv()

    def build_far(k, _):
        idx[pairs + k] = recv1[k, 3].astype(jnp.int32)
        build(pairs + k)
        return 0

    loop(0, pairs, build_far, 0, UB)

    def far_misfit(k, _):
        there = gather(table, pairs + k)
        for c in range(3):
            mis[1, k, c] = recv2[k, c] - there[c]
        return 0

    for k in range(1, pairs):
        send_mis(k, b).wait_recv()
    loop(0, pairs, far_misfit, 0, UG)
    for k in range(1, pairs):
        send_halo(k, b).wait_recv()

    def own_misfit(k, _):
        there = gather(table_of(halo.at[k], 3), 2 * pairs + k)
        for c in range(3):
            mis[0, k, c] = send2[k, c] - there[c]
        return 0

    loop(0, pairs, own_misfit, 0, UG)

    def put(slot, at_row, terms, g):
        for n, term in enumerate(terms):
            head, tail = pieces_of(term, 2)
            for t in range(tiles):
                at = slice(t * LANES, (t + 1) * LANES)
                mask = himask[g, :, at]
                both = jnp.concatenate([head[t : t + 1] * mask, tail[t : t + 1] * mask], axis=0)
                lhs[slot, at_row + rows_of * n : at_row + rows_of * (n + 1), at] = both.astype(BF16)

    def summed(totals, channel):
        at = rows_of * channel
        return totals[at : at + HI] + totals[at + HI : at + rows_of]

    def full_sum(value):
        return jnp.sum(jnp.sum(value, axis=0, keepdims=True), axis=1, keepdims=True)

    def invert(vec_ref, out_ref):
        for i in range(3):
            look = ((0, 1, 2), (1, 3, 4), (2, 4, 5))[i]
            out_ref[i] = (
                inv[look[0]] * vec_ref[0] + inv[look[1]] * vec_ref[1] + inv[look[2]] * vec_ref[2]
            )

    def exchange_start(x, table):
        for k in range(1, pairs + 1):
            k = k % pairs
            there = gather(table, pairs + k)
            for c in range(3):
                xsend[x, 1, k, c] = there[c]
            if k != 0:
                send_back(x, k, behind_of[k]).start()
        for k in range(1, pairs + 1):
            k = k % pairs
            turned = rotate(k, gather(table, k))
            for c in range(3):
                xsend[x, 0, k, c] = turned[c]
            if k != 0:
                send_ahead(x, k, ahead_of[k]).start()
        later(1, pairs, lambda k: (send_back(x, k, b).wait_send(), send_ahead(x, k, b).wait_send()))
        xrecv[x, 0, 0] = xsend[x, 0, 0]
        xrecv[x, 1, 0] = xsend[x, 1, 0]

    def send_ahead(x, k, blk):
        return copy(xsend.at[x, 0, k], xrecv.at[x, 0, k], s_x.at[x, 0, k], r_x.at[x, 0, k], blk, r)

    def send_back(x, k, blk):
        return copy(xsend.at[x, 1, k], xrecv.at[x, 1, k], s_x.at[x, 1, k], r_x.at[x, 1, k], blk, r)

    def to_twin(src, dst, send, recv):
        both = copy(src, dst, send, recv, b, 1 - r)
        both.start()
        pending.append(both.wait_send)
        return both.wait_recv

    def wait_back(x, k):
        if k != 0:
            send_back(x, k, b).wait_recv()

    def wait_ahead(x, k):
        if k != 0:
            send_ahead(x, k, b).wait_recv()

    lane = lax.broadcasted_iota(jnp.int32, (1, LANES), 1)

    def one_pass(p, _):
        def near_sums(k, totals):
            m = [mis[0, k, c] for c in range(3)]
            cf = [conf[k, c] for c in range(3)]
            squares = cf[0] * m[0] * m[0] + cf[1] * m[1] * m[1] + cf[2] * m[2] * m[2]
            weight = live[k] / jnp.sqrt(squares + SOFTEN * SOFTEN)
            wout[k] = weight
            wc = [weight * cf[c] for c in range(3)]
            for c in range(3):
                wconf[0, k, c] = wc[c]
            back = rotate_back(k, [wc[c] * m[c] for c in range(3)])
            rot = [[rotm[k, 3 * i + j] for j in range(3)] for i in range(3)]
            terms = [-value for value in back]
            for f, s in DIAGONAL + OTHERS:
                terms.append(
                    rot[0][f] * wc[0] * rot[0][s]
                    + rot[1][f] * wc[1] * rot[1][s]
                    + rot[2][f] * wc[2] * rot[2][s]
                )
            put(k, 0, terms, k)
            return totals + dot_nt(lhs[k], hot[k])

        def far_sums(k, totals):
            m = [mis[1, k, c] for c in range(3)]
            cf = [recv1[k, c] for c in range(3)]
            squares = cf[0] * m[0] * m[0] + cf[1] * m[1] * m[1] + cf[2] * m[2] * m[2]
            weight = 1.0 / jnp.sqrt(squares + SOFTEN * SOFTEN)
            wc = [weight * cf[c] for c in range(3)]
            for c in range(3):
                wconf[1, k, c] = wc[c]
            put(pairs + k, 0, [wc[c] * m[c] for c in range(3)] + wc, pairs + k)
            return totals + dot_nt(lhs[pairs + k, 0 : 6 * rows_of], hot[pairs + k])

        near = loop(0, pairs, near_sums, jnp.zeros((9 * rows_of, lo_count), F32), US)
        for n in range(6, 9):
            bsend[p, n] = summed(near, n)
        finish_others = to_twin(bsend.at[p, 6:9], brecv.at[p, 6:9], s_b.at[p, 1], r_b.at[p, 1])
        far = loop(0, pairs, far_sums, jnp.zeros((6 * rows_of, lo_count), F32), US)
        for n in range(6):
            bsend[p, n] = summed(near, n) + summed(far, n)
        finish_first = to_twin(bsend.at[p, 0:6], brecv.at[p, 0:6], s_b.at[p, 0], r_b.at[p, 0])
        finish_others()
        finish_first()
        anchor = anc[...]
        for c in range(3):
            fr[c] = bsend[p, c] + brecv[p, c] - anchor * est[c]
        diagonal = [bsend[p, 3 + n] + brecv[p, 3 + n] + anchor for n in range(3)]
        others = [bsend[p, 6 + n] + brecv[p, 6 + n] for n in range(3)]
        blocks = [diagonal[0], others[0], others[1], diagonal[1], others[2], diagonal[2]]
        adjugate = [
            blocks[3] * blocks[5] - blocks[4] * blocks[4],
            blocks[2] * blocks[4] - blocks[1] * blocks[5],
            blocks[1] * blocks[4] - blocks[2] * blocks[3],
            blocks[0] * blocks[5] - blocks[2] * blocks[2],
            blocks[1] * blocks[2] - blocks[0] * blocks[4],
            blocks[0] * blocks[3] - blocks[1] * blocks[1],
        ]
        determinant = blocks[0] * adjugate[0] + blocks[1] * adjugate[1] + blocks[2] * adjugate[2]
        for n in range(6):
            inv[n] = adjugate[n] / determinant
        invert(fr, fz)

        x = 2 * p
        exchange_start(x, table_of(fz, 2))

        def product_near(k, totals):
            wait_back(x, k)
            change = [xrecv[x, 1, k, c] - xsend[x, 0, k, c] for c in range(3)]
            pushed = []
            square = totals[1]
            for c in range(3):
                chz[0, k, c] = change[c]
                pushed.append(wconf[0, k, c] * change[c])
                square = square + pushed[c] * change[c]
            put(k, 0, [-value for value in rotate_back(k, pushed)], k)
            return totals[0] + dot_nt(lhs[k, 0 : 3 * rows_of], hot[k]), square

        def product_far(k, totals):
            wait_ahead(x, k)
            change = [xsend[x, 1, k, c] - xrecv[x, 0, k, c] for c in range(3)]
            pushed = []
            for c in range(3):
                chz[1, k, c] = change[c]
                pushed.append(wconf[1, k, c] * change[c])
            put(pairs + k, 0, pushed, pairs + k)
            return totals + dot_nt(lhs[pairs + k, 0 : 3 * rows_of], hot[pairs + k])

        zero_row = jnp.zeros((tiles, LANES), F32)
        totals, z_square = loop(
            0, pairs, product_near, (jnp.zeros((3 * rows_of, lo_count), F32), zero_row), pairs
        )
        totals = loop(0, pairs, product_far, totals, pairs)
        for c in range(3):
            dsend[p, c] = summed(totals, c)
        to_twin(dsend.at[p], drecv.at[p], s_d.at[p], r_d.at[p])()
        for c in range(3):
            fq[c] = dsend[p, c] + drecv[p, c] + anchor * fz[c]
        invert(fq, fu)

        y = 2 * p + 1
        exchange_start(y, table_of(fu, 2))

        def change_u(k, square):
            wait_back(y, k)
            for c in range(3):
                change = xrecv[y, 1, k, c] - xsend[y, 0, k, c]
                chu[k, c] = change
                square = square + wconf[0, k, c] * change * change
            return square

        u_square = loop(0, pairs, change_u, zero_row, pairs)

        half = 1.0 / n_rep
        rz = fr[0] * fz[0] + fr[1] * fz[1] + fr[2] * fz[2]
        zz = anchor * (fz[0] * fz[0] + fz[1] * fz[1] + fz[2] * fz[2])
        uu = anchor * (fu[0] * fu[0] + fu[1] * fu[1] + fu[2] * fu[2])
        uq = fu[0] * fq[0] + fu[1] * fq[1] + fu[2] * fq[2]
        parts = (
            half * full_sum(rz),
            half * full_sum(zz) + full_sum(z_square),
            half * full_sum(uq),
            half * full_sum(uu) + full_sum(u_square),
        )
        row = jnp.zeros((1, LANES), F32)
        for n, part in enumerate(parts):
            row = jnp.where(lane == n, part, row)

        def reduce_all(row, meanwhile):
            gsend[p] = row

            def start(j, _):
                pltpu.make_async_remote_copy(
                    src_ref=gsend.at[p],
                    dst_ref=grecv.at[p, me],
                    send_sem=s_g.at[p],
                    recv_sem=r_g.at[p],
                    device_id=lax.rem(me + j, count),
                    device_id_type=pl.DeviceIdType.LOGICAL,
                ).start()
                return 0

            lax.fori_loop(1, count, start, 0, unroll=UJ)
            meanwhile()
            grecv[p, me] = row
            rest = pltpu.make_async_copy(grecv.at[p, 1:count], grecv.at[p, 1:count], r_g.at[p])
            rest.wait()
            sent = pltpu.make_async_copy(grecv.at[p, 1:count], grecv.at[p, 1:count], s_g.at[p])
            pending.append(sent.wait)
            total = [grecv[p, n] for n in range(8)]
            for n in range(8, count):
                total[n % 8] = total[n % 8] + grecv[p, n]
            total = [total[n] + total[n + 4] for n in range(4)]
            return (total[0] + total[1]) + (total[2] + total[3])

        def write_weights():
            drain()
            for k in range(pairs):
                for t in range(tiles):
                    weights_out[0, k : k + 1, t * LANES : (t + 1) * LANES] = wout[k, t : t + 1]

        row = reduce_all(row, write_weights)

        def scalar(n):
            return jnp.sum(jnp.where(lane == n, row, 0.0), axis=1, keepdims=True)

        rz, zq, uq, uw = scalar(0), scalar(1), scalar(2), scalar(3)
        alpha = rz / zq
        norm_next = rz - 2.0 * alpha * zq + alpha * alpha * uq
        beta = norm_next / rz
        grown = 1.0 + beta
        along = grown * grown * zq - 2.0 * alpha * grown * uq + alpha * alpha * uw
        alpha_two = norm_next / along
        of_z = alpha + alpha_two * grown
        of_u = -alpha * alpha_two
        for c in range(3):
            est[c] = est[c] + of_z * fz[c] + of_u * fu[c]
        def new_misfit(k, _):
            wait_ahead(y, k)
            for c in range(3):
                mis[0, k, c] = mis[0, k, c] - of_z * chz[0, k, c] - of_u * chu[k, c]
                far_u = xsend[y, 1, k, c] - xrecv[y, 0, k, c]
                mis[1, k, c] = mis[1, k, c] - of_z * chz[1, k, c] - of_u * far_u
            return 0

        loop(0, pairs, new_misfit, 0, pairs)
        drain()
        return 0

    drain()
    lax.fori_loop(0, PASSES, one_pass, 0)

    for h in range(HI):
        at = slice(h * lo_count, (h + 1) * lo_count)
        for c in range(3):
            est_out[c : c + 1, at] = est[c, h : h + 1]


def on_device(
    n_blk,
    n_rep,
    measured,
    rot_vector,
    confidence,
    first_local,
    second_local,
    edge_counts,
    start_angles,
    anchor,
):
    pairs, slots = first_local.shape[1], first_local.shape[2]
    cams = start_angles.shape[1]
    tiles = slots // LANES
    lo = cams // HI
    vmem = pltpu.VMEM
    sem = pltpu.SemaphoreType.DMA

    def edges(*lead):
        return vmem((*lead, tiles, LANES), F32)

    def cameras(*lead):
        return vmem((*lead, HI, lo), F32)

    scratch = [
        vmem((3 * pairs, lo, slots), BF16),
        vmem((3 * pairs, HI, slots), F32),
        vmem((3 * pairs, tiles, LANES), jnp.int32),
        edges(pairs, 9),
        edges(pairs, 3),
        edges(pairs, 3),
        edges(pairs),
        edges(pairs),
        edges(2, pairs, 3),
        edges(2, pairs, 3),
        edges(2, pairs, 3),
        edges(pairs, 3),
        edges(pairs, 4),
        edges(pairs, 4),
        edges(pairs, 3),
        edges(pairs, 3),
        cameras(3),
        cameras(pairs, 3),
        cameras(),
        cameras(6),
        cameras(3),
        cameras(3),
        cameras(3),
        cameras(3),
        cameras(PASSES, 9),
        cameras(PASSES, 9),
        cameras(PASSES, 3),
        cameras(PASSES, 3),
        edges(2 * PASSES, 2, pairs, 3),
        edges(2 * PASSES, 2, pairs, 3),
        vmem((PASSES, 1, LANES), F32),
        vmem((PASSES, n_blk * n_rep, 1, LANES), F32),
        vmem((2 * pairs, 18 * HI, slots), BF16),
        sem((3, pairs)),
        sem((3, pairs)),
        sem((PASSES, 2)),
        sem((PASSES, 2)),
        sem((PASSES,)),
        sem((PASSES,)),
        sem((2 * PASSES, 2, pairs)),
        sem((2 * PASSES, 2, pairs)),
        sem((PASSES,)),
        sem((PASSES,)),
        vmem(measured.shape, F32),
        vmem(rot_vector.shape, F32),
        vmem(confidence.shape, F32),
        vmem(first_local.shape, jnp.int32),
        vmem(second_local.shape, jnp.int32),
        vmem((1, pairs), jnp.int32),
        vmem(start_angles.shape, F32),
        vmem((1, cams), F32),
        sem((8,)),
    ]
    whole = pl.BlockSpec(memory_space=pltpu.VMEM)
    return pl.pallas_call(
        functools.partial(kernel, n_blk, n_rep),
        out_shape=(
            pltpu.VMEM((3, cams), F32),
            pltpu.VMEM((1, pairs, slots), F32),
        ),
        in_specs=[pl.BlockSpec(memory_space=pl.ANY)] * 8,
        out_specs=(whole, whole),
        scratch_shapes=scratch,
        compiler_params=pltpu.CompilerParams(
            collective_id=0, has_side_effects=True, vmem_limit_bytes=60 * 1024 * 1024
        ),
    )(
        measured,
        rot_vector,
        confidence,
        first_local,
        second_local,
        edge_counts.reshape(1, -1),
        start_angles,
        anchor.reshape(1, -1),
    )


def solution(mesh):
    return jax.shard_map(
        functools.partial(on_device, mesh.shape["blk"], mesh.shape["rep"]),
        mesh=mesh,
        in_specs=(
            P(None, "blk", None, "rep"),
            P(None, "blk", None, "rep"),
            P(None, "blk", None, "rep"),
            P("blk", None, "rep"),
            P("blk", None, "rep"),
            P("blk", None, "rep"),
            P(None, "blk"),
            P("blk"),
        ),
        out_specs=(P(None, "blk"), P("blk", None, "rep")),
        check_vma=False,
    )
```
